32 devices in a mesh: pipe: 2 (over core), dp: 8 (over z, y), mp: 2 (over x).
Axes of the slice: x: 2, y: 2, z: 4, core: 2. Of those that a mesh axis runs over, the one named last changes fastest.
Arguments:
- token_ids: int32 [2, 4096], P('pipe', 'dp'), may hold values from 0 to 32127, as said below
- embedded: bfloat16 [2, 4096, 4096], P('pipe', 'dp', 'mp'), may hold values from -720 to 720
- norm_gain: float32 [2, 4096], P('pipe', 'mp'), may hold values from 0.25 to 1.75
- proj_grad: bfloat16 [2, 4096, 2048], P('pipe', 'dp'), may hold values from -6 to 6
- proj_weight: bfloat16 [2, 4096, 2048], P('pipe', 'mp'), may hold values from -0.125 to 0.125
- stream_grad: bfloat16 [2, 4096, 4096], P('pipe', 'dp', 'mp'), may hold values from -6 to 6
Outputs:
- table_grad: float32 [32128, 2, 2048], P('dp', 'mp', 'pipe')
The draws below stay inside these ranges and needn't reach their ends.
Inputs may be any that keep to these rules, and one draw needn't show every extreme that they name: `token_ids`: call block o the ids o * 4016 to (o + 1) * 4016 - 1. The 512 tokens of one stack on one index of dp hold at most 128 ids of any one block, and some block gets exactly 128 of them.
All inputs are finite; a program needn't handle non-finite values.
Results may differ from the reference program's by a relative error of at most 0.0029.
Values may be sent and summed in bfloat16 or wider, within the bound.
A program may use at most 128 MiB of HBM per device.

```python
import math
import jax
import jax.numpy as jnp
from jax import lax

D = 4096
VOCAB = 32128
INNER = 2048
TOK_DEV = 512
TOKENS = 4096
CAP = 128
VR = 4016
N_DP = 8


def draw_token_ids(key, part):
    hot_rows = jax.random.randint(jax.random.fold_in(key, 7), (N_DP,), 0, VR)

    def draw_block(section_number, replica):
        full_owner = jax.random.randint(jax.random.fold_in(jax.random.fold_in(key, 11), section_number), (), 0, N_DP)
        block_key = jax.random.fold_in(jax.random.fold_in(key, 101 + section_number), replica)
        key_slots, key_order, key_choose, key_rows = jax.random.split(block_key, 4)
        remaining = jax.random.permutation(key_slots, (N_DP - 1) * CAP)[:TOK_DEV - CAP]
        owners_rest = (remaining // CAP + full_owner + 1) % N_DP
        owners = jnp.concatenate([jnp.full((CAP,), full_owner, jnp.int32), owners_rest.astype(jnp.int32)])
        owners = owners[jax.random.permutation(key_order, TOK_DEV)]
        chooser = jax.random.randint(key_choose, (TOK_DEV,), 0, 4)
        uniform_rows = jax.random.randint(key_rows, (TOK_DEV,), 0, VR)
        picked = jnp.where(chooser == 0, hot_rows[owners], uniform_rows)
        return (owners * VR + picked).astype(jnp.int32)
    sections = jnp.arange(2, dtype=jnp.int32)
    replicas = jnp.arange(N_DP, dtype=jnp.int32)
    blocks = jax.vmap(lambda section_number: jax.vmap(lambda replica: draw_block(section_number, replica))(replicas))(sections)
    return blocks.reshape(2, TOKENS)


def draw_embedded(key, part):
    key_base, key_rows = jax.random.split(key, 2)
    columns = jnp.arange(D, dtype=jnp.float32) / (D - 1)
    base = jax.random.normal(key_base, (2 * TOKENS, D), jnp.float32)
    row_scale = jnp.exp(jax.random.uniform(key_rows, (2 * TOKENS, 1), jnp.float32, 0.0, math.log(10.0)))
    column_scale = jnp.exp(columns * math.log(3.0))
    base = jnp.clip(base, -5.0, 5.0)
    return (base * row_scale * column_scale[None, :]).astype(jnp.bfloat16).reshape(2, TOKENS, D)


def steps_of(rng, extent, cuts, smallest, largest):
    def one(dim, shards_of):
        draws = jax.random.uniform(jax.random.fold_in(jax.random.fold_in(rng, 6), dim), (shards_of,), jnp.float32, smallest / len(cuts), largest / len(cuts))
        return jnp.repeat(jnp.exp(draws), extent[dim] // shards_of).reshape((-1,) + (1,) * (len(extent) - dim - 1))

    factor_of = one(*cuts[0])
    for cut in cuts[1:]:
        factor_of = factor_of * one(*cut)
    return factor_of


def noise(own_key, shape, deviation, limit, shards=(), held_as=jnp.bfloat16):
    drawn = jax.random.normal(own_key, shape, jnp.float32) * deviation
    if len(shards) > 0:
        drawn = steps_of(own_key, shape, shards, -0.22, 0.18) * drawn
    return jnp.clip(drawn, min=-limit, max=limit).astype(held_as)


def setup_inputs(seed: int = 0) -> dict:
    key_of = jax.random.split(jax.random.key(seed), 7)
    token_ids = draw_token_ids(jax.random.fold_in(key_of[6], 71), 0)
    embedded = draw_embedded(jax.random.fold_in(key_of[6], 71), 0)
    norm_gain = jnp.clip(1.0 + 0.15 * jax.random.normal(key_of[2], (2, D), jnp.float32), 0.25, 1.75)
    proj_grad = noise(key_of[3], (2, TOKENS, INNER), 1.0, 6.0, ((0, 2), (1, 8)))
    proj_weight = noise(key_of[4], (2, D, INNER), INNER ** -0.5, 0.125, ((0, 2), (1, 2)))
    stream_grad = noise(key_of[5], (2, TOKENS, D), 1.0, 6.0, ((0, 2), (1, 8), (2, 2)))
    return dict(token_ids=token_ids, embedded=embedded, norm_gain=norm_gain, proj_grad=proj_grad, proj_weight=proj_weight, stream_grad=stream_grad)


epsilon = 1e-06

def stack_back(grad, weight, embed, gain, stream):
    query_back = jnp.dot(grad, weight.T, preferred_element_type=jnp.float32)
    inputs = embed.astype(jnp.float32)
    scaled = query_back * gain.astype(jnp.float32)[None, :]
    square_sum = lax.optimization_barrier(jnp.sum(inputs * inputs, axis=1))
    mixed_sum = lax.optimization_barrier(jnp.sum(inputs * scaled, axis=1))
    inverse = lax.rsqrt(square_sum / D + epsilon)
    norm_back = inverse[:, None] * scaled - inputs * (inverse * inverse * inverse * mixed_sum / D)[:, None]
    return (stream.astype(jnp.float32) + norm_back).astype(jnp.bfloat16)

def reference(token_ids, embedded, norm_gain, proj_grad, proj_weight, stream_grad):
    first = stack_back(proj_grad[0], proj_weight[0], embedded[0], norm_gain[0], stream_grad[0])
    second = stack_back(proj_grad[1], proj_weight[1], embedded[1], norm_gain[1], stream_grad[1])
    all_rows = jnp.concatenate([first, second], axis=0).astype(jnp.float32)
    table = jax.ops.segment_sum(all_rows, token_ids.reshape(-1).astype(jnp.int32), num_segments=VOCAB)
    return table.reshape(VOCAB, 2, D // 2)
```

```python
import functools

import jax
import jax.numpy as jnp
from jax import lax
from jax.experimental import pallas as pl
from jax.experimental.pallas import tpu as pltpu
from jax.sharding import PartitionSpec as P

VOCAB = 32128
LANES = 128
epsilon = 1e-06
VMEM_LIMIT = 60 * 1024 * 1024


def partner(me, k, n):
    out, bit = 0, 1
    while bit < n:
        mine = (me // bit) % 2
        flip = (k // bit) % 2
        out = out + bit * (mine + flip - 2 * mine * flip)
        bit *= 2
    return out


def contract_last(a, b):
    return lax.dot_general(a, b, (((1,), (1,)), ((), ())), preferred_element_type=jnp.float32)


def greet_all(n, pipe, other, me, mp):
    barrier = pltpu.get_barrier_semaphore()

    def greet(k, carry):
        d = partner(me, k, n)
        pl.semaphore_signal(
            barrier, inc=1, device_id={"dp": d, "pipe": other}, device_id_type=pl.DeviceIdType.MESH
        )

        @pl.when(k > 0)
        def _():
            pl.semaphore_signal(
                barrier, inc=1, device_id={"dp": d, "pipe": pipe}, device_id_type=pl.DeviceIdType.MESH
            )

        return carry

    lax.fori_loop(0, n, greet, 0)
    if mp is not None:
        pl.semaphore_signal(
            barrier, inc=1, device_id={"mp": 1 - mp}, device_id_type=pl.DeviceIdType.MESH
        )
    return barrier


def pieces_of(block_rows):
    pieces = 8
    while block_rows % pieces:
        pieces //= 2
    return pieces


def index_lanes(keep):
    return -(-keep // LANES) * LANES


def find_places(n, keep, spill, block_rows, me, ids_ref, placer_v, local_v, facts_v):
    tokens = ids_ref.shape[1]
    ids = ids_ref[...].astype(jnp.float32)
    ids_down = jnp.broadcast_to(ids, (LANES, tokens)).T[:, 0:1]
    earlier = lax.broadcasted_iota(jnp.int32, (tokens, tokens), 0) < lax.broadcasted_iota(
        jnp.int32, (tokens, tokens), 1
    )
    same = jnp.where((ids_down == ids) & earlier, 1.0, 0.0)
    first = jnp.where(jnp.sum(same, axis=0, keepdims=True) > 0.0, 0.0, 1.0)
    first_down = jnp.broadcast_to(first, (LANES, tokens)).T[:, 0:1]
    rank = jnp.sum(jnp.where(ids_down < ids, first_down, 0.0), axis=0, keepdims=True)

    k = lax.broadcasted_iota(jnp.int32, (n, 1), 0)
    low = (partner(me, k, n) * block_rows).astype(jnp.float32)

    def below(edge):
        return jnp.sum(jnp.where(ids < edge, first, 0.0), axis=1, keepdims=True)

    pieces = pieces_of(block_rows)
    base = below(low)
    bounds = [below(low + float(q * (block_rows // pieces))) - base for q in range(1, pieces + 1)]
    match = jnp.where((ids >= low) & (ids < low + float(block_rows)), 1.0, 0.0)
    rank = rank - jnp.sum(match * base, axis=0, keepdims=True)
    slot = jnp.sum(match * (k * keep).astype(jnp.float32), axis=0, keepdims=True)
    local = ids - jnp.sum(match * low, axis=0, keepdims=True)
    position = jnp.where(rank < keep, slot + rank, -1.0)
    lane = lax.broadcasted_iota(jnp.int32, (n, LANES), 1)
    facts = jnp.zeros((n, LANES), jnp.float32)
    for q in range(pieces):
        facts = jnp.where(lane == 3 + q, bounds[q], facts)
    if spill:
        over = jnp.maximum(bounds[-1] - keep, 0.0)
        start = jnp.zeros((n, 1), jnp.float32)
        for o in range(n):
            start = start + jnp.where(k > o, over[o:o + 1], 0.0)
        behind = jnp.sum(match * start, axis=0, keepdims=True) + (rank + (n * keep - keep))
        position = jnp.where(rank < keep, position, behind)
        full = jnp.where(jnp.sum(over, axis=0, keepdims=True) > spill, 1.0, 0.0)
        facts = jnp.where(lane == 0, full, jnp.where(lane == 1, start, facts))
    facts_v[...] = facts.astype(jnp.int32)
    high = jnp.floor(local * (1.0 / 64.0))
    row = lax.broadcasted_iota(jnp.int32, (8, tokens), 0)
    parts = jnp.where(row == 0, high, jnp.where(row == 1, local - high * 64.0, 0.0)) * first
    local_v[...] = parts.astype(jnp.bfloat16)
    slots = lax.broadcasted_iota(jnp.int32, placer_v.shape, 0)
    placer_v[...] = jnp.where(position.astype(jnp.int32) == slots, 1.0, 0.0).astype(jnp.bfloat16)


def place_indices(n, keep, spill, placer_v, local_v, facts_v, sendi_v):
    parts = contract_last(local_v[...], placer_v[...])
    found = (parts[0:1] * 64.0 + parts[1:2]).astype(jnp.int32)
    facts_at = sendi_v.shape[2] - LANES
    sendi_v[...] = jnp.zeros(sendi_v.shape, jnp.int32)
    for k in range(n):
        sendi_v[k, :, 0:keep] = found[:, k * keep:(k + 1) * keep]
        if spill:
            sendi_v[k, :, facts_at - LANES:facts_at] = found[:, n * keep:]
        sendi_v[k, :, facts_at:] = facts_v[k:k + 1, :]


def place_rows(c, chunk, keep, spill, placer_v, part, send_v, over_v):
    n, _, _, half = send_v.shape
    p, cols = c * chunk // half, pl.ds(c * chunk % half, chunk)
    placed = jnp.dot(
        placer_v[0:n * keep + spill, :], part, preferred_element_type=jnp.float32
    ).astype(jnp.bfloat16)
    send_v[:, p, :, cols] = placed[:n * keep].reshape(n, keep, chunk)
    if spill:
        over_v[p, :, cols] = placed[n * keep:]


def remote(src, dst, send_sem, recv_sem, **where):
    return pltpu.make_async_remote_copy(
        src_ref=src, dst_ref=dst, send_sem=send_sem, recv_sem=recv_sem,
        device_id=where, device_id_type=pl.DeviceIdType.MESH,
    )


def make_sender(n, pipe, other, me, send_v, sendi_v, rows_out, index_out, sems):
    send_sem, recv_sem, isend_sem, irecv_sem = sems

    def copies(k, p, s):
        d = partner(me, k, n)
        return (
            remote(send_v.at[k, p], rows_out.at[k, s], send_sem.at[k, p], recv_sem.at[k, s], dp=d, pipe=p),
            remote(sendi_v.at[k], index_out.at[k, s], isend_sem.at[k, p], irecv_sem.at[k, s], dp=d, pipe=p),
        )

    def send(k, own_chip):
        for copy in copies(k, other, pipe):
            copy.start()
        if not own_chip:
            for copy in copies(k, pipe, pipe):
                copy.start()

    def arrive(k, carry):
        for copy in copies(k, other, pipe):
            copy.wait_send()
        for copy in copies(k, other, other):
            copy.wait_recv()

        @pl.when(k > 0)
        def _():
            for copy in copies(k, pipe, pipe):
                copy.wait_send()
            for copy in copies(k, other, pipe):
                copy.wait_recv()

        return carry

    return send, arrive


def exchange_kernel(
    n, cap, keep, spill, block_rows, full_width, chunk,
    ids_ref, gain_ref, embedded, proj_grad, weight, stream,
    rows_out, index_out, spill_out, kept_out,
    emb_v, grad_v, weight_v, stream_v, scaled_v, rows_v, send_v, sendi_v, over_v, sums_v, sums_got,
    placer_v, local_v, facts_v,
    in_sem, weight_sem, sum_send, sum_recv, send_sem, recv_sem, isend_sem, irecv_sem, own_sem,
    pair_send, pair_recv, line_send, line_recv, side_send, side_recv,
):
    pipe = lax.axis_index("pipe")
    me = lax.axis_index("dp")
    mp = lax.axis_index("mp")
    other = 1 - pipe
    tokens, width = emb_v.shape
    half = width // 2

    loads = [
        pltpu.make_async_copy(proj_grad, grad_v, in_sem.at[0]),
        pltpu.make_async_copy(embedded, emb_v, in_sem.at[1]),
        pltpu.make_async_copy(stream, stream_v, in_sem.at[2]),
    ]
    chunks = [
        pltpu.make_async_copy(
            weight.at[pl.ds(j * chunk, chunk)], weight_v.at[pl.ds(j * chunk, chunk)], weight_sem.at[j]
        )
        for j in range(width // chunk)
    ]
    loads[0].start()
    chunks[0].start()
    loads[1].start()
    for copy in chunks[1:]:
        copy.start()
    loads[2].start()
    barrier = greet_all(n, pipe, other, me, mp)
    find_places(n, keep, spill, block_rows, me, ids_ref, placer_v, local_v, facts_v)

    loads[0].wait()
    mixed = jnp.zeros((tokens, 1), jnp.float32)
    square = jnp.zeros((tokens, 1), jnp.float32)
    for j in range(width // chunk):
        cols = pl.ds(j * chunk, chunk)
        chunks[j].wait()
        if j == 0:
            loads[1].wait()
        scaled = contract_last(grad_v[...], weight_v[cols, :]) * gain_ref[:, cols]
        scaled_v[:, cols] = scaled
        inputs = emb_v[:, cols].astype(jnp.float32)
        square = square + jnp.sum(inputs * inputs, axis=1, keepdims=True)
        mixed = mixed + jnp.sum(inputs * scaled, axis=1, keepdims=True)
    lane = lax.broadcasted_iota(jnp.int32, (tokens, LANES), 1)
    packed = jnp.where(lane == 0, square, jnp.where(lane == 1, mixed, 0.0))
    sums_v[...] = packed.T[:8]

    pl.semaphore_wait(barrier, 2 * n)
    swap = remote(sums_v, sums_got, sum_send, sum_recv, mp=1 - mp)
    swap.start()
    place_indices(n, keep, spill, placer_v, local_v, facts_v, sendi_v)
    loads[2].wait()
    swap.wait()

    total = sums_v[...] + sums_got[...]
    inverse = lax.rsqrt(total[0:1] / full_width + epsilon)
    coef = inverse * inverse * inverse * total[1:2] / full_width
    line = lax.broadcasted_iota(jnp.int32, (LANES, tokens), 0)
    back = jnp.where(line == 0, inverse, jnp.where(line == 1, coef, 0.0)).T
    for j in range(width // chunk):
        cols = pl.ds(j * chunk, chunk)
        norm_back = back[:, 0:1] * scaled_v[:, cols] - emb_v[:, cols].astype(jnp.float32) * back[:, 1:2]
        part = (stream_v[:, cols].astype(jnp.float32) + norm_back).astype(jnp.bfloat16)
        if spill:
            rows_v[:, cols] = part
        place_rows(j, chunk, keep, spill, placer_v, part, send_v, over_v)

    send, arrive = make_sender(
        n, pipe, other, me, send_v, sendi_v, rows_out, index_out,
        (send_sem, recv_sem, isend_sem, irecv_sem),
    )
    if spill:
        lines = n // 2
        at, beside = me // 2, partner(me, 1, n)
        pair = remote(over_v.at[other], spill_out.at[0, pipe], pair_send, pair_recv, pipe=other)
        pair.start()
        own_over = pltpu.make_async_copy(over_v.at[pipe], spill_out.at[0, pipe], own_sem.at[2])
        own_over.start()
        kept = pltpu.make_async_copy(rows_v, kept_out, own_sem.at[3])
        kept.start()

        def along(up, r, source, to):
            return remote(
                spill_out.at[partner(me, source, n)], spill_out.at[partner(to, source, n)],
                line_send.at[up, r], line_recv.at[up, r], dp=to,
            )

        def across(source):
            return remote(
                spill_out.at[partner(me, source, n)], spill_out.at[partner(beside, source, n)],
                side_send.at[source // 2], side_recv.at[source // 2], dp=beside,
            )

        def pass_on(r):
            for up in (1, 0):
                step = 2 if up else -2
                source = me - step * r
                here = (at >= r) if up else (at + r < lines)
                more = (at + 1 < lines) if up else (at >= 1)
                if r > 0:

                    @pl.when(here)
                    def _():
                        remote(
                            spill_out.at[0], spill_out.at[partner(me, source, n)],
                            line_send.at[up, r], line_recv.at[up, r], dp=beside,
                        ).wait_recv()
                        across(source).start()

                @pl.when(here & more)
                def _():
                    along(up, r + 1, source, me + step).start()

            if r == 0:
                across(me).start()

        def finish(r):
            for up in (1, 0):
                step = 2 if up else -2
                source = me - step * r
                here = (at >= r) if up else (at + r < lines)
                more = (at + 1 < lines) if up else (at >= 1)

                @pl.when(here & more)
                def _():
                    along(up, r + 1, source, me + step).wait_send()

        send(1, False)
        own_over.wait()
        pair.wait()
        pass_on(0)
        for k in range(2, n):
            send(k, False)
            if k % 2 == 1 and k // 2 < lines:
                pass_on(k // 2)
        send(0, True)
    else:

        def send_on(k, carry):
            send(k, False)
            return carry

        lax.fori_loop(1, n, send_on, 0)
        send(0, True)
    own_rows = pltpu.make_async_copy(send_v.at[0, pipe], rows_out.at[0, pipe], own_sem.at[0])
    own_index = pltpu.make_async_copy(sendi_v.at[0], index_out.at[0, pipe], own_sem.at[1])
    own_rows.start()
    own_index.start()
    lax.fori_loop(0, n, arrive, 0)
    own_rows.wait()
    own_index.wait()
    if spill:
        for r in range(lines):
            finish(r)

        def side(z, carry):
            remote(
                spill_out.at[partner(me, 2 * z, n)], spill_out.at[partner(me, 2 * z + beside % 2, n)],
                side_send.at[z], side_recv.at[z], dp=beside,
            ).wait()
            return carry

        lax.fori_loop(0, lines, side, 0)
        kept.wait()


def exchange(ids, embedded, gain, proj_grad, weight, stream, n, n_mp, cap, keep, spill, block_rows):
    tokens, width = embedded.shape
    inner = proj_grad.shape[1]
    half = width // 2
    chunk = min(256, half)
    index_width = index_lanes(keep) + (2 * LANES if spill else LANES)
    over = (spill or 16, half)
    kept = (tokens, width) if spill else (8, LANES)
    any_space = pl.BlockSpec(memory_space=pl.ANY)
    vmem = pl.BlockSpec(memory_space=pltpu.VMEM)
    dma = pltpu.SemaphoreType.DMA
    return pl.pallas_call(
        functools.partial(exchange_kernel, n, cap, keep, spill, block_rows, width * n_mp, chunk),
        out_shape=(
            jax.ShapeDtypeStruct((n, 2, keep, half), jnp.bfloat16),
            jax.ShapeDtypeStruct((n, 2, 1, index_width), jnp.int32),
            jax.ShapeDtypeStruct((n if spill else 1, 2) + over, jnp.bfloat16),
            jax.ShapeDtypeStruct(kept, jnp.bfloat16),
        ),
        in_specs=[vmem, vmem] + [any_space] * 4,
        out_specs=(any_space,) * 4,
        scratch_shapes=[
            pltpu.VMEM((tokens, width), jnp.bfloat16),
            pltpu.VMEM((tokens, inner), jnp.bfloat16),
            pltpu.VMEM((width, inner), jnp.bfloat16),
            pltpu.VMEM((tokens, width), jnp.bfloat16),
            pltpu.VMEM((tokens, width), jnp.float32),
            pltpu.VMEM((tokens, width), jnp.bfloat16),
            pltpu.VMEM((n, 2, keep, half), jnp.bfloat16),
            pltpu.VMEM((n, 1, index_width), jnp.int32),
            pltpu.VMEM((2,) + over, jnp.bfloat16),
            pltpu.VMEM((8, tokens), jnp.float32),
            pltpu.VMEM((8, tokens), jnp.float32),
            pltpu.VMEM((n * keep + (LANES if spill else 0), tokens), jnp.bfloat16),
            pltpu.VMEM((8, tokens), jnp.bfloat16),
            pltpu.VMEM((n, LANES), jnp.int32),
            dma((3,)),
            dma((width // chunk,)),
            dma,
            dma,
            dma((n, 2)),
            dma((n, 2)),
            dma((n, 2)),
            dma((n, 2)),
            dma((4,)),
            dma,
            dma,
            dma((2, n)),
            dma((2, n)),
            dma((n,)),
            dma((n,)),
        ],
        compiler_params=pltpu.CompilerParams(
            collective_id=0, has_side_effects=True, vmem_limit_bytes=VMEM_LIMIT
        ),
    )(ids, gain, embedded, proj_grad, weight, stream)


def full_kernel(
    n, cap, block_rows, ids_ref, rows_v, rows_out, index_out, send_v, sendi_v, placer_v, local_v, facts_v,
    send_sem, recv_sem, isend_sem, irecv_sem, own_sem,
):
    pipe = lax.axis_index("pipe")
    me = lax.axis_index("dp")
    other = 1 - pipe
    barrier = greet_all(n, pipe, other, me, None)
    pl.semaphore_wait(barrier, 2 * n - 1)
    find_places(n, cap, 0, block_rows, me, ids_ref, placer_v, local_v, facts_v)
    place_indices(n, cap, 0, placer_v, local_v, facts_v, sendi_v)
    width = rows_v.shape[1]
    chunk = min(256, width // 2)
    for c in range(width // chunk):
        place_rows(c, chunk, cap, 0, placer_v, rows_v[:, c * chunk:(c + 1) * chunk], send_v, None)
    send, arrive = make_sender(
        n, pipe, other, me, send_v, sendi_v, rows_out, index_out,
        (send_sem, recv_sem, isend_sem, irecv_sem),
    )

    def send_on(k, carry):
        send(k, False)
        return carry

    lax.fori_loop(1, n, send_on, 0)
    send(0, True)
    own_rows = pltpu.make_async_copy(send_v.at[0, pipe], rows_out.at[0, pipe], own_sem.at[0])
    own_index = pltpu.make_async_copy(sendi_v.at[0], index_out.at[0, pipe], own_sem.at[1])
    own_rows.start()
    own_index.start()
    lax.fori_loop(0, n, arrive, 0)
    own_rows.wait()
    own_index.wait()


def full_exchange(ids, rows, n, cap, block_rows):
    tokens, width = rows.shape
    half = width // 2
    any_space = pl.BlockSpec(memory_space=pl.ANY)
    vmem = pl.BlockSpec(memory_space=pltpu.VMEM)
    dma = pltpu.SemaphoreType.DMA
    return pl.pallas_call(
        functools.partial(full_kernel, n, cap, block_rows),
        out_shape=(
            jax.ShapeDtypeStruct((n, 2, cap, half), jnp.bfloat16),
            jax.ShapeDtypeStruct((n, 2, 1, index_lanes(cap) + LANES), jnp.int32),
        ),
        in_specs=[vmem, vmem],
        out_specs=(any_space, any_space),
        scratch_shapes=[
            pltpu.VMEM((n, 2, cap, half), jnp.bfloat16),
            pltpu.VMEM((n, 1, index_lanes(cap) + LANES), jnp.int32),
            pltpu.VMEM((n * cap, tokens), jnp.bfloat16),
            pltpu.VMEM((8, tokens), jnp.bfloat16),
            pltpu.VMEM((n, LANES), jnp.int32),
            dma((n, 2)),
            dma((n, 2)),
            dma((n, 2)),
            dma((n, 2)),
            dma((2,)),
        ],
        compiler_params=pltpu.CompilerParams(
            collective_id=1, has_side_effects=True, vmem_limit_bytes=VMEM_LIMIT
        ),
    )(ids, rows)


def table_kernel(spilled, pieces, index_ref, rows_ref, *rest):
    if spilled:
        over_ref, out_ref, wide_v, over_v = rest[:4]
        tables, sem = rest[4:-1], rest[-1]
    else:
        out_ref, wide_v = rest[:2]
        tables, sem = rest[2:-1], rest[-1]
    blocks, keep, half = rows_ref.shape
    lines = half // LANES
    piece_rows = out_ref.shape[0] // (pieces * lines)
    facts_at = index_ref.shape[2] - LANES
    batch = 8

    def widen(b, carry):
        for j in range(lines):
            wide_v[pl.ds(b * keep * lines + j, keep, stride=lines), :] = rows_ref[
                b, :, j * LANES:(j + 1) * LANES
            ].astype(jnp.float32)
        if spilled:

            @pl.when(index_ref[b, 0, facts_at + 2 + pieces] > keep)
            def _():
                for j in range(lines):
                    over_v[pl.ds(b * spilled * lines + j, spilled, stride=lines), :] = over_ref[
                        b, :, j * LANES:(j + 1) * LANES
                    ].astype(jnp.float32)

        return carry

    lax.fori_loop(0, blocks, widen, 0)

    def add_rows(table_v, source_v, b, size, index_from, first_row, start, stop):
        def add(g, carry):
            olds, news, places = [], [], []
            for u in range(batch):
                c = start + g * batch + u
                here = c < stop
                c = jnp.minimum(c, size - 1)
                v = jnp.where(here, index_ref[b, 0, index_from + c] - first_row, piece_rows)
                places.append(pl.multiple_of(v * lines, lines))
                olds.append(table_v[pl.ds(places[u], lines), :])
                news.append(source_v[pl.ds(pl.multiple_of((b * size + c) * lines, lines), lines), :])
            for u in range(batch):
                table_v[pl.ds(places[u], lines), :] = olds[u] + news[u]
            return carry

        lax.fori_loop(0, (stop - start + (batch - 1)) // batch, add, 0)

    copies = []
    for q in range(pieces):
        table_v = tables[q]
        table_v[...] = jnp.zeros(table_v.shape, jnp.float32)

        def block(b, carry):
            low = index_ref[b, 0, facts_at + 2 + q]
            high = index_ref[b, 0, facts_at + 3 + q]
            if spilled:
                low_kept, high_kept = jnp.minimum(low, keep), jnp.minimum(high, keep)
            else:
                low_kept, high_kept = low, high
            add_rows(table_v, wide_v, b, keep, 0, q * piece_rows, low_kept, high_kept)
            if spilled:
                begin = index_ref[b, 0, facts_at + 1]
                add_rows(
                    table_v, over_v, b, spilled, facts_at - LANES, q * piece_rows,
                    begin + low - low_kept, begin + high - high_kept,
                )
            return carry

        lax.fori_loop(0, blocks, block, 0)
        span = piece_rows * lines
        copies.append(
            pltpu.make_async_copy(table_v.at[pl.ds(0, span)], out_ref.at[pl.ds(q * span, span)], sem.at[q])
        )
        copies[q].start()
    for copy in copies:
        copy.wait()


def table(index, rows, over, block_rows):
    n, stacks, keep, half = rows.shape
    lines = half // LANES
    blocks = n * stacks
    pieces = pieces_of(block_rows)
    spilled = 0 if over is None else over.shape[2]
    vmem = pl.BlockSpec(memory_space=pltpu.VMEM)
    operands = [index.reshape(blocks, 1, -1), rows.reshape(blocks, keep, half)]
    in_specs = [pl.BlockSpec(memory_space=pltpu.SMEM), vmem]
    scratch = [pltpu.VMEM((blocks * keep * lines, LANES), jnp.float32)]
    if spilled:
        operands.append(over.reshape(blocks, spilled, half))
        in_specs.append(vmem)
        scratch.append(pltpu.VMEM((blocks * spilled * lines, LANES), jnp.float32))
    scratch += [pltpu.VMEM(((block_rows // pieces + 1) * lines, LANES), jnp.float32)] * pieces
    scratch.append(pltpu.SemaphoreType.DMA((pieces,)))
    return pl.pallas_call(
        functools.partial(table_kernel, spilled, pieces),
        out_shape=jax.ShapeDtypeStruct((block_rows * lines, LANES), jnp.float32),
        in_specs=in_specs,
        out_specs=pl.BlockSpec(memory_space=pl.ANY),
        scratch_shapes=scratch,
        compiler_params=pltpu.CompilerParams(vmem_limit_bytes=VMEM_LIMIT),
    )(*operands)


def on_device(token_ids, embedded, norm_gain, proj_grad, proj_weight, stream_grad):
    n = lax.axis_size("dp")
    tokens = token_ids.shape[1]
    cap = max(2, 2 * tokens // n)
    block_rows = VOCAB // n
    tiers = cap == LANES
    keep = 3 * cap // 8 if tiers else cap
    spill = 5 * cap // 8 if tiers else 0
    rows, index, over, kept = exchange(
        token_ids, embedded[0], norm_gain, proj_grad[0], proj_weight[0], stream_grad[0],
        n, lax.axis_size("mp"), cap, keep, spill, block_rows,
    )
    half = rows.shape[-1]
    if tiers:

        def whole():
            full_rows, full_index = full_exchange(token_ids, kept, n, cap, block_rows)
            return table(full_index, full_rows, None, block_rows)

        def short():
            return table(index, rows, over, block_rows)

        out = lax.cond(jnp.max(index[:, :, 0, index.shape[-1] - LANES]) > 0, whole, short)
    else:
        out = table(index, rows, None, block_rows)
    return out.reshape(block_rows, 1, half)


def solution(mesh):
    return jax.shard_map(
        on_device,
        mesh=mesh,
        in_specs=(
            P("pipe", "dp"),
            P("pipe", "dp", "mp"),
            P("pipe", "mp"),
            P("pipe", "dp", None),
            P("pipe", "mp", None),
            P("pipe", "dp", "mp"),
        ),
        out_specs=P("dp", "mp", "pipe"),
        check_vma=False,
    )
```

```python
import functools

import jax
import jax.numpy as jnp
from jax import lax
from jax.experimental import pallas as pl
from jax.experimental.pallas import tpu as pltpu
from jax.sharding import PartitionSpec as P

VOCAB = 32128
LANES = 128
epsilon = 1e-06
BATCH = 8
VMEM_LIMIT = 60 * 1024 * 1024


def partner(me, k, n):
    out, bit = 0, 1
    while bit < n:
        mine = (me // bit) % 2
        flip = (k // bit) % 2
        out = out + bit * (mine + flip - 2 * mine * flip)
        bit *= 2
    return out


def contract_last(a, b):
    return lax.dot_general(a, b, (((1,), (1,)), ((), ())), preferred_element_type=jnp.float32)


def greet_all(n, pipe, other, me, mp):
    barrier = pltpu.get_barrier_semaphore()

    def greet(k, carry):
        d = partner(me, k, n)
        pl.semaphore_signal(
            barrier, inc=1, device_id={"dp": d, "pipe": other}, device_id_type=pl.DeviceIdType.MESH
        )

        @pl.when(k > 0)
        def _():
            pl.semaphore_signal(
                barrier, inc=1, device_id={"dp": d, "pipe": pipe}, device_id_type=pl.DeviceIdType.MESH
            )

        return carry

    lax.fori_loop(0, n, greet, 0)
    if mp is not None:
        pl.semaphore_signal(
            barrier, inc=1, device_id={"mp": 1 - mp}, device_id_type=pl.DeviceIdType.MESH
        )
    return barrier


def pieces_of(block_rows):
    pieces = 8
    while block_rows % pieces:
        pieces //= 2
    return pieces


def index_lanes(keep):
    return -(-keep // LANES) * LANES


def batches(count):
    return jnp.floor((count + (BATCH - 1)) * (1.0 / BATCH))


def find_places(n, keep, spill, block_rows, me, ids_ref, placer_v, local_v, facts_v):
    tokens = ids_ref.shape[1]
    ids = ids_ref[...].astype(jnp.float32)
    ids_down = jnp.broadcast_to(ids, (LANES, tokens)).T[:, 0:1]
    earlier = lax.broadcasted_iota(jnp.int32, (tokens, tokens), 0) < lax.broadcasted_iota(
        jnp.int32, (tokens, tokens), 1
    )
    same = jnp.where((ids_down == ids) & earlier, 1.0, 0.0)
    first = jnp.where(jnp.sum(same, axis=0, keepdims=True) > 0.0, 0.0, 1.0)
    first_down = jnp.broadcast_to(first, (LANES, tokens)).T[:, 0:1]
    rank = jnp.sum(jnp.where(ids_down < ids, first_down, 0.0), axis=0, keepdims=True)

    k = lax.broadcasted_iota(jnp.int32, (n, 1), 0)
    low = (partner(me, k, n) * block_rows).astype(jnp.float32)

    def below(edge):
        return jnp.sum(jnp.where(ids < edge, first, 0.0), axis=1, keepdims=True)

    pieces = pieces_of(block_rows)
    base = below(low)
    bounds = [below(low + float(q * (block_rows // pieces))) - base for q in range(1, pieces + 1)]
    match = jnp.where((ids >= low) & (ids < low + float(block_rows)), 1.0, 0.0)
    rank = rank - jnp.sum(match * base, axis=0, keepdims=True)
    slot = jnp.sum(match * (k * keep).astype(jnp.float32), axis=0, keepdims=True)
    local = ids - jnp.sum(match * low, axis=0, keepdims=True)
    position = jnp.where(rank < keep, slot + rank, -1.0)
    lane = lax.broadcasted_iota(jnp.int32, (n, LANES), 1)
    facts = jnp.zeros((n, LANES), jnp.float32)
    for q in range(pieces):
        facts = jnp.where(lane == 2 + q, batches(jnp.minimum(bounds[q], keep)), facts)
    if spill:
        over = jnp.maximum(bounds[-1] - keep, 0.0)
        start = jnp.zeros((n, 1), jnp.float32)
        for o in range(n):
            start = start + jnp.where(k > o, over[o:o + 1], 0.0)
        behind = jnp.sum(match * start, axis=0, keepdims=True) + (rank + (n * keep - keep))
        position = jnp.where(rank < keep, position, behind)
        full = jnp.where(jnp.sum(over, axis=0, keepdims=True) > spill, 1.0, 0.0)
        begin = jnp.floor(start * (1.0 / BATCH))
        facts = jnp.where(lane == 0, full, jnp.where(lane == 1, begin, facts))
        for q in range(pieces):
            passed = jnp.maximum(bounds[q] - keep, 0.0)
            passed = jnp.where(passed > 0.0, batches(start + passed), begin)
            facts = jnp.where(lane == 2 + pieces + q, jnp.minimum(passed, float(spill // BATCH)), facts)
    facts_v[...] = facts.astype(jnp.int32)
    high = jnp.floor(local * (1.0 / 64.0))
    row = lax.broadcasted_iota(jnp.int32, (8, tokens), 0)
    parts = jnp.where(row == 0, high, jnp.where(row == 1, local - high * 64.0, 0.0))
    owner = jnp.sum(match * (k + 1).astype(jnp.float32), axis=0, keepdims=True)
    parts = jnp.where(row == 2, owner, parts) * first
    local_v[...] = parts.astype(jnp.bfloat16)
    slots = lax.broadcasted_iota(jnp.int32, placer_v.shape, 0)
    placer_v[...] = jnp.where(position.astype(jnp.int32) == slots, 1.0, 0.0).astype(jnp.bfloat16)


def place_indices(n, keep, spill, block_rows, lines, placer_v, local_v, facts_v, sendi_v):
    parts = contract_last(local_v[...], placer_v[...])
    owner = parts[2:3]
    found = parts[0:1] * 64.0 + parts[1:2]
    found = jnp.where(owner > 0.0, found, float(block_rows))
    found = (found * float(lines)).astype(jnp.int32)
    facts_at = sendi_v.shape[2] - LANES
    sendi_v[...] = jnp.zeros(sendi_v.shape, jnp.int32)
    for k in range(n):
        sendi_v[k, :, 0:keep] = found[:, k * keep:(k + 1) * keep]
        if spill:
            sendi_v[k, :, facts_at - LANES:facts_at] = jnp.where(
                owner[:, n * keep:] == float(k + 1), found[:, n * keep:], block_rows * lines
            )
        sendi_v[k, :, facts_at:] = facts_v[k:k + 1, :]


def place_rows(c, chunk, keep, spill, placer_v, part, send_v, over_v):
    n, _, _, half = send_v.shape
    p, cols = c * chunk // half, pl.ds(c * chunk % half, chunk)
    placed = jnp.dot(
        placer_v[0:n * keep + spill, :], part, preferred_element_type=jnp.float32
    ).astype(jnp.bfloat16)
    send_v[:, p, :, cols] = placed[:n * keep].reshape(n, keep, chunk)
    if spill:
        over_v[p, :, cols] = placed[n * keep:]


def remote(src, dst, send_sem, recv_sem, **where):
    return pltpu.make_async_remote_copy(
        src_ref=src, dst_ref=dst, send_sem=send_sem, recv_sem=recv_sem,
        device_id=where, device_id_type=pl.DeviceIdType.MESH,
    )


def make_sender(n, pipe, other, me, send_v, sendi_v, rows_out, index_out, sems):
    send_sem, recv_sem, isend_sem, irecv_sem = sems

    def copies(k, p, s):
        d = partner(me, k, n)
        return (
            remote(send_v.at[k, p], rows_out.at[k, s], send_sem.at[k, p], recv_sem.at[k, s], dp=d, pipe=p),
            remote(sendi_v.at[k], index_out.at[k, s], isend_sem.at[k, p], irecv_sem.at[k, s], dp=d, pipe=p),
        )

    def send(k, own_chip):
        for copy in copies(k, other, pipe):
            copy.start()
        if not own_chip:
            for copy in copies(k, pipe, pipe):
                copy.start()

    def arrive(k, carry):
        for copy in copies(k, other, pipe):
            copy.wait_send()
        for copy in copies(k, other, other):
            copy.wait_recv()

        @pl.when(k > 0)
        def _():
            for copy in copies(k, pipe, pipe):
                copy.wait_send()
            for copy in copies(k, other, pipe):
                copy.wait_recv()

        return carry

    return send, arrive


def exchange_kernel(
    n, cap, keep, spill, block_rows, full_width, chunk,
    ids_ref, gain_ref, embedded, proj_grad, weight, stream,
    rows_out, index_out, spill_out, kept_out,
    emb_v, grad_v, weight_v, stream_v, scaled_v, rows_v, send_v, sendi_v, over_v, sums_v, sums_got,
    placer_v, local_v, facts_v,
    in_sem, weight_sem, sum_send, sum_recv, send_sem, recv_sem, isend_sem, irecv_sem, own_sem,
    pair_send, pair_recv, line_send, line_recv, side_send, side_recv,
):
    pipe = lax.axis_index("pipe")
    me = lax.axis_index("dp")
    mp = lax.axis_index("mp")
    other = 1 - pipe
    tokens, width = emb_v.shape
    half = width // 2

    loads = [
        pltpu.make_async_copy(proj_grad, grad_v, in_sem.at[0]),
        pltpu.make_async_copy(embedded, emb_v, in_sem.at[1]),
        pltpu.make_async_copy(stream, stream_v, in_sem.at[2]),
    ]
    chunks = [
        pltpu.make_async_copy(
            weight.at[pl.ds(j * chunk, chunk)], weight_v.at[pl.ds(j * chunk, chunk)], weight_sem.at[j]
        )
        for j in range(width // chunk)
    ]
    loads[0].start()
    chunks[0].start()
    loads[1].start()
    for copy in chunks[1:]:
        copy.start()
    loads[2].start()
    barrier = greet_all(n, pipe, other, me, mp)
    find_places(n, keep, spill, block_rows, me, ids_ref, placer_v, local_v, facts_v)

    loads[0].wait()
    mixed = jnp.zeros((tokens, 1), jnp.float32)
    square = jnp.zeros((tokens, 1), jnp.float32)
    for j in range(width // chunk):
        cols = pl.ds(j * chunk, chunk)
        chunks[j].wait()
        if j == 0:
            loads[1].wait()
        scaled = contract_last(grad_v[...], weight_v[cols, :]) * gain_ref[:, cols]
        scaled_v[:, cols] = scaled
        inputs = emb_v[:, cols].astype(jnp.float32)
        square = square + jnp.sum(inputs * inputs, axis=1, keepdims=True)
        mixed = mixed + jnp.sum(inputs * scaled, axis=1, keepdims=True)
    lane = lax.broadcasted_iota(jnp.int32, (tokens, LANES), 1)
    packed = jnp.where(lane == 0, square, jnp.where(lane == 1, mixed, 0.0))
    sums_v[...] = packed.T[:8]

    pl.semaphore_wait(barrier, 2 * n)
    swap = remote(sums_v, sums_got, sum_send, sum_recv, mp=1 - mp)
    swap.start()
    place_indices(n, keep, spill, block_rows, half // LANES, placer_v, local_v, facts_v, sendi_v)
    loads[2].wait()
    swap.wait()

    total = sums_v[...] + sums_got[...]
    inverse = lax.rsqrt(total[0:1] / full_width + epsilon)
    coef = inverse * inverse * inverse * total[1:2] / full_width
    line = lax.broadcasted_iota(jnp.int32, (LANES, tokens), 0)
    back = jnp.where(line == 0, inverse, jnp.where(line == 1, coef, 0.0)).T
    for j in range(width // chunk):
        cols = pl.ds(j * chunk, chunk)
        norm_back = back[:, 0:1] * scaled_v[:, cols] - emb_v[:, cols].astype(jnp.float32) * back[:, 1:2]
        part = (stream_v[:, cols].astype(jnp.float32) + norm_back).astype(jnp.bfloat16)
        if spill:
            rows_v[:, cols] = part
        place_rows(j, chunk, keep, spill, placer_v, part, send_v, over_v)

    send, arrive = make_sender(
        n, pipe, other, me, send_v, sendi_v, rows_out, index_out,
        (send_sem, recv_sem, isend_sem, irecv_sem),
    )
    if spill:
        lines = n // 2
        at, beside = me // 2, partner(me, 1, n)
        pair = remote(over_v.at[other], spill_out.at[0, pipe], pair_send, pair_recv, pipe=other)
        pair.start()
        own_over = pltpu.make_async_copy(over_v.at[pipe], spill_out.at[0, pipe], own_sem.at[2])
        own_over.start()
        kept = pltpu.make_async_copy(rows_v, kept_out, own_sem.at[3])
        kept.start()

        def along(up, r, source, to):
            return remote(
                spill_out.at[partner(me, source, n)], spill_out.at[partner(to, source, n)],
                line_send.at[up, r], line_recv.at[up, r], dp=to,
            )

        def across(source):
            return remote(
                spill_out.at[partner(me, source, n)], spill_out.at[partner(beside, source, n)],
                side_send.at[source // 2], side_recv.at[source // 2], dp=beside,
            )

        def pass_on(r):
            for up in (1, 0):
                step = 2 if up else -2
                source = me - step * r
                here = (at >= r) if up else (at + r < lines)
                more = (at + 1 < lines) if up else (at >= 1)
                if r > 0:

                    @pl.when(here)
                    def _():
                        remote(
                            spill_out.at[0], spill_out.at[partner(me, source, n)],
                            line_send.at[up, r], line_recv.at[up, r], dp=beside,
                        ).wait_recv()
                        across(source).start()

                @pl.when(here & more)
                def _():
                    along(up, r + 1, source, me + step).start()

            if r == 0:
                across(me).start()

        def finish(r):
            for up in (1, 0):
                step = 2 if up else -2
                source = me - step * r
                here = (at >= r) if up else (at + r < lines)
                more = (at + 1 < lines) if up else (at >= 1)

                @pl.when(here & more)
                def _():
                    along(up, r + 1, source, me + step).wait_send()

        send(1, False)
        own_over.wait()
        pair.wait()
        pass_on(0)
        for k in range(2, n):
            send(k, False)
            if k % 2 == 1 and k // 2 < lines:
                pass_on(k // 2)
        send(0, True)
    else:

        def send_on(k, carry):
            send(k, False)
            return carry

        lax.fori_loop(1, n, send_on, 0)
        send(0, True)
    own_rows = pltpu.make_async_copy(send_v.at[0, pipe], rows_out.at[0, pipe], own_sem.at[0])
    own_index = pltpu.make_async_copy(sendi_v.at[0], index_out.at[0, pipe], own_sem.at[1])
    own_rows.start()
    own_index.start()
    lax.fori_loop(0, n, arrive, 0)
    own_rows.wait()
    own_index.wait()
    if spill:
        for r in range(lines):
            finish(r)

        def side(z, carry):
            remote(
                spill_out.at[partner(me, 2 * z, n)], spill_out.at[partner(me, 2 * z + beside % 2, n)],
                side_send.at[z], side_recv.at[z], dp=beside,
            ).wait()
            return carry

        lax.fori_loop(0, lines, side, 0)
        kept.wait()


def exchange(ids, embedded, gain, proj_grad, weight, stream, n, n_mp, cap, keep, spill, block_rows):
    tokens, width = embedded.shape
    inner = proj_grad.shape[1]
    half = width // 2
    chunk = min(256, half)
    index_width = index_lanes(keep) + (2 * LANES if spill else LANES)
    over = (spill or 16, half)
    kept = (tokens, width) if spill else (8, LANES)
    any_space = pl.BlockSpec(memory_space=pl.ANY)
    vmem = pl.BlockSpec(memory_space=pltpu.VMEM)
    dma = pltpu.SemaphoreType.DMA
    return pl.pallas_call(
        functools.partial(exchange_kernel, n, cap, keep, spill, block_rows, width * n_mp, chunk),
        out_shape=(
            jax.ShapeDtypeStruct((n, 2, keep, half), jnp.bfloat16),
            jax.ShapeDtypeStruct((n, 2, 1, index_width), jnp.int32),
            jax.ShapeDtypeStruct((n if spill else 1, 2) + over, jnp.bfloat16),
            jax.ShapeDtypeStruct(kept, jnp.bfloat16),
        ),
        in_specs=[vmem, vmem] + [any_space] * 4,
        out_specs=(any_space,) * 4,
        scratch_shapes=[
            pltpu.VMEM((tokens, width), jnp.bfloat16),
            pltpu.VMEM((tokens, inner), jnp.bfloat16),
            pltpu.VMEM((width, inner), jnp.bfloat16),
            pltpu.VMEM((tokens, width), jnp.bfloat16),
            pltpu.VMEM((tokens, width), jnp.float32),
            pltpu.VMEM((tokens, width), jnp.bfloat16),
            pltpu.VMEM((n, 2, keep, half), jnp.bfloat16),
            pltpu.VMEM((n, 1, index_width), jnp.int32),
            pltpu.VMEM((2,) + over, jnp.bfloat16),
            pltpu.VMEM((8, tokens), jnp.float32),
            pltpu.VMEM((8, tokens), jnp.float32),
            pltpu.VMEM((n * keep + (LANES if spill else 0), tokens), jnp.bfloat16),
            pltpu.VMEM((8, tokens), jnp.bfloat16),
            pltpu.VMEM((n, LANES), jnp.int32),
            dma((3,)),
            dma((width // chunk,)),
            dma,
            dma,
            dma((n, 2)),
            dma((n, 2)),
            dma((n, 2)),
            dma((n, 2)),
            dma((4,)),
            dma,
            dma,
            dma((2, n)),
            dma((2, n)),
            dma((n,)),
            dma((n,)),
        ],
        compiler_params=pltpu.CompilerParams(
            collective_id=0, has_side_effects=True, vmem_limit_bytes=VMEM_LIMIT
        ),
    )(ids, gain, embedded, proj_grad, weight, stream)


def full_kernel(
    n, cap, block_rows, ids_ref, rows_v, rows_out, index_out, send_v, sendi_v, placer_v, local_v, facts_v,
    send_sem, recv_sem, isend_sem, irecv_sem, own_sem,
):
    pipe = lax.axis_index("pipe")
    me = lax.axis_index("dp")
    other = 1 - pipe
    barrier = greet_all(n, pipe, other, me, None)
    pl.semaphore_wait(barrier, 2 * n - 1)
    find_places(n, cap, 0, block_rows, me, ids_ref, placer_v, local_v, facts_v)
    width = rows_v.shape[1]
    place_indices(n, cap, 0, block_rows, width // 2 // LANES, placer_v, local_v, facts_v, sendi_v)
    chunk = min(256, width // 2)
    for c in range(width // chunk):
        place_rows(c, chunk, cap, 0, placer_v, rows_v[:, c * chunk:(c + 1) * chunk], send_v, None)
    send, arrive = make_sender(
        n, pipe, other, me, send_v, sendi_v, rows_out, index_out,
        (send_sem, recv_sem, isend_sem, irecv_sem),
    )

    def send_on(k, carry):
        send(k, False)
        return carry

    lax.fori_loop(1, n, send_on, 0)
    send(0, True)
    own_rows = pltpu.make_async_copy(send_v.at[0, pipe], rows_out.at[0, pipe], own_sem.at[0])
    own_index = pltpu.make_async_copy(sendi_v.at[0], index_out.at[0, pipe], own_sem.at[1])
    own_rows.start()
    own_index.start()
    lax.fori_loop(0, n, arrive, 0)
    own_rows.wait()
    own_index.wait()


def full_exchange(ids, rows, n, cap, block_rows):
    tokens, width = rows.shape
    half = width // 2
    any_space = pl.BlockSpec(memory_space=pl.ANY)
    vmem = pl.BlockSpec(memory_space=pltpu.VMEM)
    dma = pltpu.SemaphoreType.DMA
    return pl.pallas_call(
        functools.partial(full_kernel, n, cap, block_rows),
        out_shape=(
            jax.ShapeDtypeStruct((n, 2, cap, half), jnp.bfloat16),
            jax.ShapeDtypeStruct((n, 2, 1, index_lanes(cap) + LANES), jnp.int32),
        ),
        in_specs=[vmem, vmem],
        out_specs=(any_space, any_space),
        scratch_shapes=[
            pltpu.VMEM((n, 2, cap, half), jnp.bfloat16),
            pltpu.VMEM((n, 1, index_lanes(cap) + LANES), jnp.int32),
            pltpu.VMEM((n * cap, tokens), jnp.bfloat16),
            pltpu.VMEM((8, tokens), jnp.bfloat16),
            pltpu.VMEM((n, LANES), jnp.int32),
            dma((n, 2)),
            dma((n, 2)),
            dma((n, 2)),
            dma((n, 2)),
            dma((2,)),
        ],
        compiler_params=pltpu.CompilerParams(
            collective_id=1, has_side_effects=True, vmem_limit_bytes=VMEM_LIMIT
        ),
    )(ids, rows)


def table_kernel(spilled, pieces, index_ref, rows_ref, *rest):
    if spilled:
        over_ref, out_ref, wide_v, over_v, table_v, sem = rest
    else:
        out_ref, wide_v, table_v, sem = rest
    blocks, keep, half = rows_ref.shape
    lines = half // LANES
    span = out_ref.shape[0] // pieces
    facts_at = index_ref.shape[2] - LANES
    parts = 16
    while out_ref.shape[0] % (8 * parts):
        parts //= 2
    clear_rows = out_ref.shape[0] // parts

    def clear(i, carry):
        table_v[pl.ds(pl.multiple_of(i * clear_rows, 8), clear_rows), :] = jnp.zeros(
            (clear_rows, LANES), jnp.float32
        )
        return carry

    lax.fori_loop(0, parts, clear, 0)

    def widen(b, carry):
        for j in range(lines):
            wide_v[pl.ds(b * keep * lines + j, keep, stride=lines), :] = rows_ref[
                b, :, j * LANES:(j + 1) * LANES
            ].astype(jnp.float32)
        if spilled:

            @pl.when(index_ref[b, 0, facts_at + 1 + 2 * pieces] > index_ref[b, 0, facts_at + 1])
            def _():
                for j in range(lines):
                    over_v[pl.ds(b * spilled * lines + j, spilled, stride=lines), :] = over_ref[
                        b, :, j * LANES:(j + 1) * LANES
                    ].astype(jnp.float32)

        return carry

    lax.fori_loop(0, blocks, widen, 0)

    def add_rows(source_v, b, size, index_from, start, stop):
        def add(g, carry):
            first = g * BATCH
            place = pl.multiple_of((b * size + first) * lines, BATCH * lines)
            places = [
                pl.multiple_of(index_ref[b, 0, index_from + first + u], lines) for u in range(BATCH)
            ]
            sums = [
                table_v[pl.ds(places[u], lines), :] + source_v[pl.ds(place + u * lines, lines), :]
                for u in range(BATCH)
            ]
            for u in range(BATCH):
                table_v[pl.ds(places[u], lines), :] = sums[u]
            return carry

        lax.fori_loop(start, stop, add, 0)

    copies = []
    for q in range(pieces):

        def block(b, carry):
            start = index_ref[b, 0, facts_at + 1 + q] if q else 0
            add_rows(wide_v, b, keep, 0, start, index_ref[b, 0, facts_at + 2 + q])
            if spilled:
                start = index_ref[b, 0, facts_at + (1 + pieces + q if q else 1)]
                add_rows(
                    over_v, b, spilled, facts_at - LANES, start,
                    index_ref[b, 0, facts_at + 2 + pieces + q],
                )
            return carry

        lax.fori_loop(0, blocks, block, 0)
        rows = pl.ds(q * span, span)
        copies.append(pltpu.make_async_copy(table_v.at[rows], out_ref.at[rows], sem.at[q]))
        copies[q].start()
    for copy in copies:
        copy.wait()


def table(index, rows, over, block_rows):
    n, stacks, keep, half = rows.shape
    lines = half // LANES
    blocks = n * stacks
    pieces = pieces_of(block_rows)
    spilled = 0 if over is None else over.shape[2]
    vmem = pl.BlockSpec(memory_space=pltpu.VMEM)
    operands = [index.reshape(blocks, 1, -1), rows.reshape(blocks, keep, half)]
    in_specs = [pl.BlockSpec(memory_space=pltpu.SMEM), vmem]
    scratch = [pltpu.VMEM((blocks * keep * lines, LANES), jnp.float32)]
    if spilled:
        operands.append(over.reshape(blocks, spilled, half))
        in_specs.append(vmem)
        scratch.append(pltpu.VMEM((blocks * spilled * lines, LANES), jnp.float32))
    scratch.append(pltpu.VMEM(((block_rows + 1) * lines, LANES), jnp.float32))
    scratch.append(pltpu.SemaphoreType.DMA((pieces,)))
    return pl.pallas_call(
        functools.partial(table_kernel, spilled, pieces),
        out_shape=jax.ShapeDtypeStruct((block_rows * lines, LANES), jnp.float32),
        in_specs=in_specs,
        out_specs=pl.BlockSpec(memory_space=pl.ANY),
        scratch_shapes=scratch,
        compiler_params=pltpu.CompilerParams(vmem_limit_bytes=VMEM_LIMIT),
    )(*operands)


def on_device(token_ids, embedded, norm_gain, proj_grad, proj_weight, stream_grad):
    n = lax.axis_size("dp")
    tokens = token_ids.shape[1]
    cap = max(2, 2 * tokens // n)
    block_rows = VOCAB // n
    tiers = cap == LANES
    keep = 3 * cap // 8 if tiers else cap
    spill = 5 * cap // 8 if tiers else 0
    rows, index, over, kept = exchange(
        token_ids, embedded[0], norm_gain, proj_grad[0], proj_weight[0], stream_grad[0],
        n, lax.axis_size("mp"), cap, keep, spill, block_rows,
    )
    half = rows.shape[-1]
    if tiers:

        def whole():
            full_rows, full_index = full_exchange(token_ids, kept, n, cap, block_rows)
            return table(full_index, full_rows, None, block_rows)

        def short():
            return table(index, rows, over, block_rows)

        out = lax.cond(jnp.max(index[:, :, 0, index.shape[-1] - LANES]) > 0, whole, short)
    else:
        out = table(index, rows, None, block_rows)
    return out.reshape(block_rows, 1, half)


def solution(mesh):
    return jax.shard_map(
        on_device,
        mesh=mesh,
        in_specs=(
            P("pipe", "dp"),
            P("pipe", "dp", "mp"),
            P("pipe", "mp"),
            P("pipe", "dp", None),
            P("pipe", "mp", None),
            P("pipe", "dp", "mp"),
        ),
        out_specs=P("dp", "mp", "pipe"),
        check_vma=False,
    )
```

```python
import functools

import jax
import jax.numpy as jnp
from jax import lax
from jax.experimental import pallas as pl
from jax.experimental.pallas import tpu as pltpu
from jax.sharding import PartitionSpec as P

VOCAB = 32128
LANES = 128
epsilon = 1e-06
BATCH = 8
VMEM_LIMIT = 60 * 1024 * 1024


def partner(me, k, n):
    out, bit = 0, 1
    while bit < n:
        mine = (me // bit) % 2
        flip = (k // bit) % 2
        out = out + bit * (mine + flip - 2 * mine * flip)
        bit *= 2
    return out


def contract_last(a, b):
    return lax.dot_general(a, b, (((1,), (1,)), ((), ())), preferred_element_type=jnp.float32)


def greet_all(n, pipe, other, me, mp):
    barrier = pltpu.get_barrier_semaphore()

    def greet(k, carry):
        d = partner(me, k, n)
        pl.semaphore_signal(
            barrier, inc=1, device_id={"dp": d, "pipe": other}, device_id_type=pl.DeviceIdType.MESH
        )

        @pl.when(k > 0)
        def _():
            pl.semaphore_signal(
                barrier, inc=1, device_id={"dp": d, "pipe": pipe}, device_id_type=pl.DeviceIdType.MESH
            )

        return carry

    lax.fori_loop(0, n, greet, 0)
    if mp is not None:
        pl.semaphore_signal(
            barrier, inc=1, device_id={"mp": 1 - mp}, device_id_type=pl.DeviceIdType.MESH
        )
    return barrier


def pieces_of(block_rows):
    pieces = 8
    while block_rows % pieces:
        pieces //= 2
    return pieces


def index_lanes(keep):
    return -(-keep // LANES) * LANES


def batches(count):
    return jnp.floor((count + (BATCH - 1)) * (1.0 / BATCH))


def find_places(n, keep, spill, block_rows, me, ids_ref, placer_v, local_v, facts_v):
    tokens = ids_ref.shape[1]
    ids = ids_ref[...].astype(jnp.float32)
    ids_down = jnp.broadcast_to(ids, (LANES, tokens)).T[:, 0:1]
    earlier = lax.broadcasted_iota(jnp.int32, (tokens, tokens), 0) < lax.broadcasted_iota(
        jnp.int32, (tokens, tokens), 1
    )
    same = jnp.where((ids_down == ids) & earlier, 1.0, 0.0)
    first = jnp.where(jnp.sum(same, axis=0, keepdims=True) > 0.0, 0.0, 1.0)
    first_down = jnp.broadcast_to(first, (LANES, tokens)).T[:, 0:1]
    rank = jnp.sum(jnp.where(ids_down < ids, first_down, 0.0), axis=0, keepdims=True)

    k = lax.broadcasted_iota(jnp.int32, (n, 1), 0)
    low = (partner(me, k, n) * block_rows).astype(jnp.float32)

    def below(edge):
        return jnp.sum(jnp.where(ids < edge, first, 0.0), axis=1, keepdims=True)

    pieces = pieces_of(block_rows)
    base = below(low)
    bounds = [below(low + float(q * (block_rows // pieces))) - base for q in range(1, pieces + 1)]
    match = jnp.where((ids >= low) & (ids < low + float(block_rows)), 1.0, 0.0)
    rank = rank - jnp.sum(match * base, axis=0, keepdims=True)
    slot = jnp.sum(match * (k * keep).astype(jnp.float32), axis=0, keepdims=True)
    local = ids - jnp.sum(match * low, axis=0, keepdims=True)
    position = jnp.where(rank < keep, slot + rank, -1.0)
    lane = lax.broadcasted_iota(jnp.int32, (n, LANES), 1)
    facts = jnp.zeros((n, LANES), jnp.float32)
    for q in range(pieces):
        facts = jnp.where(lane == 2 + q, batches(jnp.minimum(bounds[q], keep)), facts)
    if spill:
        over = jnp.maximum(bounds[-1] - keep, 0.0)
        start = jnp.zeros((n, 1), jnp.float32)
        for o in range(n):
            start = start + jnp.where(k > o, over[o:o + 1], 0.0)
        behind = jnp.sum(match * start, axis=0, keepdims=True) + (rank + (n * keep - keep))
        position = jnp.where(rank < keep, position, behind)
        full = jnp.where(jnp.sum(over, axis=0, keepdims=True) > spill, 1.0, 0.0)
        begin = jnp.floor(start * (1.0 / BATCH))
        facts = jnp.where(lane == 0, full, jnp.where(lane == 1, begin, facts))
        for q in range(pieces):
            passed = jnp.maximum(bounds[q] - keep, 0.0)
            passed = jnp.where(passed > 0.0, batches(start + passed), begin)
            facts = jnp.where(lane == 2 + pieces + q, jnp.minimum(passed, float(spill // BATCH)), facts)
    facts_v[...] = facts.astype(jnp.int32)
    high = jnp.floor(local * (1.0 / 64.0))
    row = lax.broadcasted_iota(jnp.int32, (8, tokens), 0)
    parts = jnp.where(row == 0, high, jnp.where(row == 1, local - high * 64.0, 0.0))
    owner = jnp.sum(match * (k + 1).astype(jnp.float32), axis=0, keepdims=True)
    parts = jnp.where(row == 2, owner, parts) * first
    local_v[...] = parts.astype(jnp.bfloat16)
    slots = lax.broadcasted_iota(jnp.int32, placer_v.shape, 0)
    placer_v[...] = jnp.where(position.astype(jnp.int32) == slots, 1.0, 0.0).astype(jnp.bfloat16)


def place_indices(n, keep, spill, block_rows, lines, placer_v, local_v, facts_v, sendi_v):
    parts = contract_last(local_v[...], placer_v[...])
    owner = parts[2:3]
    found = parts[0:1] * 64.0 + parts[1:2]
    found = jnp.where(owner > 0.0, found, float(block_rows))
    found = (found * float(lines)).astype(jnp.int32)
    facts_at = sendi_v.shape[2] - LANES
    sendi_v[...] = jnp.zeros(sendi_v.shape, jnp.int32)
    for k in range(n):
        sendi_v[k, :, 0:keep] = found[:, k * keep:(k + 1) * keep]
        if spill:
            sendi_v[k, :, facts_at - LANES:facts_at] = jnp.where(
                owner[:, n * keep:] == float(k + 1), found[:, n * keep:], block_rows * lines
            )
        sendi_v[k, :, facts_at:] = facts_v[k:k + 1, :]


def place_rows(c, chunk, keep, spill, placer_v, part, send_v, over_v):
    n, _, _, half = send_v.shape
    p, cols = c * chunk // half, pl.ds(c * chunk % half, chunk)
    placed = jnp.dot(
        placer_v[0:n * keep + spill, :], part, preferred_element_type=jnp.float32
    ).astype(jnp.bfloat16)
    send_v[:, p, :, cols] = placed[:n * keep].reshape(n, keep, chunk)
    if spill:
        over_v[p, :, cols] = placed[n * keep:]


def remote(src, dst, send_sem, recv_sem, **where):
    return pltpu.make_async_remote_copy(
        src_ref=src, dst_ref=dst, send_sem=send_sem, recv_sem=recv_sem,
        device_id=where, device_id_type=pl.DeviceIdType.MESH,
    )


def make_sender(n, pipe, other, me, send_v, sendi_v, rows_out, index_out, sems):
    send_sem, recv_sem, isend_sem, irecv_sem = sems

    def copies(k, p, s):
        d = partner(me, k, n)
        return (
            remote(send_v.at[k, p], rows_out.at[k, s], send_sem.at[k, p], recv_sem.at[k, s], dp=d, pipe=p),
            remote(sendi_v.at[k], index_out.at[k, s], isend_sem.at[k, p], irecv_sem.at[k, s], dp=d, pipe=p),
        )

    def send(k, own_chip):
        for copy in copies(k, other, pipe):
            copy.start()
        if not own_chip:
            for copy in copies(k, pipe, pipe):
                copy.start()

    def arrive(k, carry):
        for copy in copies(k, other, pipe):
            copy.wait_send()
        for copy in copies(k, other, other):
            copy.wait_recv()

        @pl.when(k > 0)
        def _():
            for copy in copies(k, pipe, pipe):
                copy.wait_send()
            for copy in copies(k, other, pipe):
                copy.wait_recv()

        return carry

    return send, arrive


def exchange_kernel(
    n, cap, keep, spill, block_rows, full_width, chunk,
    ids_ref, gain_ref, embedded, proj_grad, weight, stream,
    rows_out, index_out, spill_out, kept_out,
    emb_v, grad_v, weight_v, stream_v, scaled_v, rows_v, send_v, sendi_v, over_v, sums_v, sums_got,
    placer_v, local_v, facts_v,
    in_sem, weight_sem, sum_send, sum_recv, send_sem, recv_sem, isend_sem, irecv_sem, own_sem,
    pair_send, pair_recv, line_send, line_recv, side_send, side_recv,
):
    pipe = lax.axis_index("pipe")
    me = lax.axis_index("dp")
    mp = lax.axis_index("mp")
    other = 1 - pipe
    tokens, width = emb_v.shape
    half = width // 2

    loads = [
        pltpu.make_async_copy(proj_grad, grad_v, in_sem.at[0]),
        pltpu.make_async_copy(embedded, emb_v, in_sem.at[1]),
        pltpu.make_async_copy(stream, stream_v, in_sem.at[2]),
    ]
    chunks = [
        pltpu.make_async_copy(
            weight.at[pl.ds(j * chunk, chunk)], weight_v.at[pl.ds(j * chunk, chunk)], weight_sem.at[j]
        )
        for j in range(width // chunk)
    ]
    loads[0].start()
    chunks[0].start()
    barrier = greet_all(n, pipe, other, me, mp)
    find_places(n, keep, spill, block_rows, me, ids_ref, placer_v, local_v, facts_v)
    chunks[1].start()
    loads[1].start()

    loads[0].wait()
    mixed = jnp.zeros((tokens, 1), jnp.float32)
    square = jnp.zeros((tokens, 1), jnp.float32)
    for j in range(width // chunk):
        cols = pl.ds(j * chunk, chunk)
        if j + 2 < width // chunk:
            chunks[j + 2].start()
        else:
            loads[2].start() if j + 2 == width // chunk else None
        chunks[j].wait()
        scaled = contract_last(grad_v[...], weight_v[cols, :]) * gain_ref[:, cols]
        scaled_v[:, cols] = scaled
        if j == 0:
            loads[1].wait()
        inputs = emb_v[:, cols].astype(jnp.float32)
        square = square + jnp.sum(inputs * inputs, axis=1, keepdims=True)
        mixed = mixed + jnp.sum(inputs * scaled, axis=1, keepdims=True)
    lane = lax.broadcasted_iota(jnp.int32, (tokens, LANES), 1)
    packed = jnp.where(lane == 0, square, jnp.where(lane == 1, mixed, 0.0))
    sums_v[...] = packed.T[:8]

    pl.semaphore_wait(barrier, 2 * n)
    swap = remote(sums_v, sums_got, sum_send, sum_recv, mp=1 - mp)
    swap.start()
    place_indices(n, keep, spill, block_rows, half // LANES, placer_v, local_v, facts_v, sendi_v)
    loads[2].wait()
    swap.wait()

    total = sums_v[...] + sums_got[...]
    inverse = lax.rsqrt(total[0:1] / full_width + epsilon)
    coef = inverse * inverse * inverse * total[1:2] / full_width
    line = lax.broadcasted_iota(jnp.int32, (LANES, tokens), 0)
    back = jnp.where(line == 0, inverse, jnp.where(line == 1, coef, 0.0)).T
    for j in range(width // chunk):
        cols = pl.ds(j * chunk, chunk)
        norm_back = back[:, 0:1] * scaled_v[:, cols] - emb_v[:, cols].astype(jnp.float32) * back[:, 1:2]
        part = (stream_v[:, cols].astype(jnp.float32) + norm_back).astype(jnp.bfloat16)
        if spill:
            rows_v[:, cols] = part
        place_rows(j, chunk, keep, spill, placer_v, part, send_v, over_v)

    send, arrive = make_sender(
        n, pipe, other, me, send_v, sendi_v, rows_out, index_out,
        (send_sem, recv_sem, isend_sem, irecv_sem),
    )
    if spill:
        lines = n // 2
        at, beside = me // 2, partner(me, 1, n)
        pair = remote(over_v.at[other], spill_out.at[0, pipe], pair_send, pair_recv, pipe=other)
        pair.start()
        own_over = pltpu.make_async_copy(over_v.at[pipe], spill_out.at[0, pipe], own_sem.at[2])
        own_over.start()
        kept = pltpu.make_async_copy(rows_v, kept_out, own_sem.at[3])
        kept.start()

        def along(up, r, source, to):
            return remote(
                spill_out.at[partner(me, source, n)], spill_out.at[partner(to, source, n)],
                line_send.at[up, r], line_recv.at[up, r], dp=to,
            )

        def across(source):
            return remote(
                spill_out.at[partner(me, source, n)], spill_out.at[partner(beside, source, n)],
                side_send.at[source // 2], side_recv.at[source // 2], dp=beside,
            )

        def pass_on(r):
            for up in (1, 0):
                step = 2 if up else -2
                source = me - step * r
                here = (at >= r) if up else (at + r < lines)
                more = (at + 1 < lines) if up else (at >= 1)
                if r > 0:

                    @pl.when(here)
                    def _():
                        remote(
                            spill_out.at[0], spill_out.at[partner(me, source, n)],
                            line_send.at[up, r], line_recv.at[up, r], dp=beside,
                        ).wait_recv()
                        across(source).start()

                @pl.when(here & more)
                def _():
                    along(up, r + 1, source, me + step).start()

            if r == 0:
                across(me).start()

        def finish(r):
            for up in (1, 0):
                step = 2 if up else -2
                source = me - step * r
                here = (at >= r) if up else (at + r < lines)
                more = (at + 1 < lines) if up else (at >= 1)

                @pl.when(here & more)
                def _():
                    along(up, r + 1, source, me + step).wait_send()

        send(1, False)
        own_over.wait()
        pair.wait()
        pass_on(0)
        for k in range(2, n):
            send(k, False)
            if k % 2 == 1 and k // 2 < lines:
                pass_on(k // 2)
        send(0, True)
    else:

        def send_on(k, carry):
            send(k, False)
            return carry

        lax.fori_loop(1, n, send_on, 0)
        send(0, True)
    own_rows = pltpu.make_async_copy(send_v.at[0, pipe], rows_out.at[0, pipe], own_sem.at[0])
    own_index = pltpu.make_async_copy(sendi_v.at[0], index_out.at[0, pipe], own_sem.at[1])
    own_rows.start()
    own_index.start()
    lax.fori_loop(0, n, arrive, 0)
    own_rows.wait()
    own_index.wait()
    if spill:
        for r in range(lines):
            finish(r)

        def side(z, carry):
            remote(
                spill_out.at[partner(me, 2 * z, n)], spill_out.at[partner(me, 2 * z + beside % 2, n)],
                side_send.at[z], side_recv.at[z], dp=beside,
            ).wait()
            return carry

        lax.fori_loop(0, lines, side, 0)
        kept.wait()


def exchange(ids, embedded, gain, proj_grad, weight, stream, n, n_mp, cap, keep, spill, block_rows):
    tokens, width = embedded.shape
    inner = proj_grad.shape[1]
    half = width // 2
    chunk = min(512, half)
    index_width = index_lanes(keep) + (2 * LANES if spill else LANES)
    over = (spill or 16, half)
    kept = (tokens, width) if spill else (8, LANES)
    any_space = pl.BlockSpec(memory_space=pl.ANY)
    vmem = pl.BlockSpec(memory_space=pltpu.VMEM)
    dma = pltpu.SemaphoreType.DMA
    return pl.pallas_call(
        functools.partial(exchange_kernel, n, cap, keep, spill, block_rows, width * n_mp, chunk),
        out_shape=(
            jax.ShapeDtypeStruct((n, 2, keep, half), jnp.bfloat16),
            jax.ShapeDtypeStruct((n, 2, 1, index_width), jnp.int32),
            jax.ShapeDtypeStruct((n if spill else 1, 2) + over, jnp.bfloat16),
            jax.ShapeDtypeStruct(kept, jnp.bfloat16),
        ),
        in_specs=[vmem, vmem] + [any_space] * 4,
        out_specs=(any_space,) * 4,
        scratch_shapes=[
            pltpu.VMEM((tokens, width), jnp.bfloat16),
            pltpu.VMEM((tokens, inner), jnp.bfloat16),
            pltpu.VMEM((width, inner), jnp.bfloat16),
            pltpu.VMEM((tokens, width), jnp.bfloat16),
            pltpu.VMEM((tokens, width), jnp.float32),
            pltpu.VMEM((tokens, width), jnp.bfloat16),
            pltpu.VMEM((n, 2, keep, half), jnp.bfloat16),
            pltpu.VMEM((n, 1, index_width), jnp.int32),
            pltpu.VMEM((2,) + over, jnp.bfloat16),
            pltpu.VMEM((8, tokens), jnp.float32),
            pltpu.VMEM((8, tokens), jnp.float32),
            pltpu.VMEM((n * keep + (LANES if spill else 0), tokens), jnp.bfloat16),
            pltpu.VMEM((8, tokens), jnp.bfloat16),
            pltpu.VMEM((n, LANES), jnp.int32),
            dma((3,)),
            dma((width // chunk,)),
            dma,
            dma,
            dma((n, 2)),
            dma((n, 2)),
            dma((n, 2)),
            dma((n, 2)),
            dma((4,)),
            dma,
            dma,
            dma((2, n)),
            dma((2, n)),
            dma((n,)),
            dma((n,)),
        ],
        compiler_params=pltpu.CompilerParams(
            collective_id=0, has_side_effects=True, vmem_limit_bytes=VMEM_LIMIT
        ),
    )(ids, gain, embedded, proj_grad, weight, stream)


def full_kernel(
    n, cap, block_rows, ids_ref, rows_v, rows_out, index_out, send_v, sendi_v, placer_v, local_v, facts_v,
    send_sem, recv_sem, isend_sem, irecv_sem, own_sem,
):
    pipe = lax.axis_index("pipe")
    me = lax.axis_index("dp")
    other = 1 - pipe
    barrier = greet_all(n, pipe, other, me, None)
    pl.semaphore_wait(barrier, 2 * n - 1)
    find_places(n, cap, 0, block_rows, me, ids_ref, placer_v, local_v, facts_v)
    width = rows_v.shape[1]
    place_indices(n, cap, 0, block_rows, width // 2 // LANES, placer_v, local_v, facts_v, sendi_v)
    chunk = min(256, width // 2)
    for c in range(width // chunk):
        place_rows(c, chunk, cap, 0, placer_v, rows_v[:, c * chunk:(c + 1) * chunk], send_v, None)
    send, arrive = make_sender(
        n, pipe, other, me, send_v, sendi_v, rows_out, index_out,
        (send_sem, recv_sem, isend_sem, irecv_sem),
    )

    def send_on(k, carry):
        send(k, False)
        return carry

    lax.fori_loop(1, n, send_on, 0)
    send(0, True)
    own_rows = pltpu.make_async_copy(send_v.at[0, pipe], rows_out.at[0, pipe], own_sem.at[0])
    own_index = pltpu.make_async_copy(sendi_v.at[0], index_out.at[0, pipe], own_sem.at[1])
    own_rows.start()
    own_index.start()
    lax.fori_loop(0, n, arrive, 0)
    own_rows.wait()
    own_index.wait()


def full_exchange(ids, rows, n, cap, block_rows):
    tokens, width = rows.shape
    half = width // 2
    any_space = pl.BlockSpec(memory_space=pl.ANY)
    vmem = pl.BlockSpec(memory_space=pltpu.VMEM)
    dma = pltpu.SemaphoreType.DMA
    return pl.pallas_call(
        functools.partial(full_kernel, n, cap, block_rows),
        out_shape=(
            jax.ShapeDtypeStruct((n, 2, cap, half), jnp.bfloat16),
            jax.ShapeDtypeStruct((n, 2, 1, index_lanes(cap) + LANES), jnp.int32),
        ),
        in_specs=[vmem, vmem],
        out_specs=(any_space, any_space),
        scratch_shapes=[
            pltpu.VMEM((n, 2, cap, half), jnp.bfloat16),
            pltpu.VMEM((n, 1, index_lanes(cap) + LANES), jnp.int32),
            pltpu.VMEM((n * cap, tokens), jnp.bfloat16),
            pltpu.VMEM((8, tokens), jnp.bfloat16),
            pltpu.VMEM((n, LANES), jnp.int32),
            dma((n, 2)),
            dma((n, 2)),
            dma((n, 2)),
            dma((n, 2)),
            dma((2,)),
        ],
        compiler_params=pltpu.CompilerParams(
            collective_id=1, has_side_effects=True, vmem_limit_bytes=VMEM_LIMIT
        ),
    )(ids, rows)


def table_kernel(spilled, pieces, index_ref, rows_ref, *rest):
    if spilled:
        over_ref, out_ref, wide_v, over_v, table_v, sem = rest
    else:
        out_ref, wide_v, table_v, sem = rest
    blocks, keep, half = rows_ref.shape
    lines = half // LANES
    span = out_ref.shape[0] // pieces
    facts_at = index_ref.shape[2] - LANES
    parts = 16
    while out_ref.shape[0] % (8 * parts):
        parts //= 2
    clear_rows = out_ref.shape[0] // parts

    def clear(i, carry):
        table_v[pl.ds(pl.multiple_of(i * clear_rows, 8), clear_rows), :] = jnp.zeros(
            (clear_rows, LANES), jnp.float32
        )
        return carry

    lax.fori_loop(0, parts, clear, 0)

    def widen(b, carry):
        for j in range(lines):
            wide_v[pl.ds(b * keep * lines + j, keep, stride=lines), :] = rows_ref[
                b, :, j * LANES:(j + 1) * LANES
            ].astype(jnp.float32)
        if spilled:

            @pl.when(index_ref[b, 0, facts_at + 1 + 2 * pieces] > index_ref[b, 0, facts_at + 1])
            def _():
                for j in range(lines):
                    over_v[pl.ds(b * spilled * lines + j, spilled, stride=lines), :] = over_ref[
                        b, :, j * LANES:(j + 1) * LANES
                    ].astype(jnp.float32)

        return carry

    lax.fori_loop(0, blocks, widen, 0)

    def add_rows(source_v, b, size, index_from, start, stop):
        def add(g, carry):
            first = g * BATCH
            place = pl.multiple_of((b * size + first) * lines, BATCH * lines)
            places = [
                pl.multiple_of(index_ref[b, 0, index_from + first + u], lines) for u in range(BATCH)
            ]
            sums = [
                table_v[pl.ds(places[u], lines), :] + source_v[pl.ds(place + u * lines, lines), :]
                for u in range(BATCH)
            ]
            for u in range(BATCH):
                table_v[pl.ds(places[u], lines), :] = sums[u]
            return carry

        lax.fori_loop(start, stop, add, 0)

    copies = []
    for q in range(pieces):

        def block(b, carry):
            start = index_ref[b, 0, facts_at + 1 + q] if q else 0
            add_rows(wide_v, b, keep, 0, start, index_ref[b, 0, facts_at + 2 + q])
            if spilled:
                start = index_ref[b, 0, facts_at + (1 + pieces + q if q else 1)]
                add_rows(
                    over_v, b, spilled, facts_at - LANES, start,
                    index_ref[b, 0, facts_at + 2 + pieces + q],
                )
            return carry

        lax.fori_loop(0, blocks, block, 0)
        rows = pl.ds(q * span, span)
        copies.append(pltpu.make_async_copy(table_v.at[rows], out_ref.at[rows], sem.at[q]))
        copies[q].start()
    for copy in copies:
        copy.wait()


def table(index, rows, over, block_rows):
    n, stacks, keep, half = rows.shape
    lines = half // LANES
    blocks = n * stacks
    pieces = pieces_of(block_rows)
    spilled = 0 if over is None else over.shape[2]
    vmem = pl.BlockSpec(memory_space=pltpu.VMEM)
    operands = [index.reshape(blocks, 1, -1), rows.reshape(blocks, keep, half)]
    in_specs = [pl.BlockSpec(memory_space=pltpu.SMEM), vmem]
    scratch = [pltpu.VMEM((blocks * keep * lines, LANES), jnp.float32)]
    if spilled:
        operands.append(over.reshape(blocks, spilled, half))
        in_specs.append(vmem)
        scratch.append(pltpu.VMEM((blocks * spilled * lines, LANES), jnp.float32))
    scratch.append(pltpu.VMEM(((block_rows + 1) * lines, LANES), jnp.float32))
    scratch.append(pltpu.SemaphoreType.DMA((pieces,)))
    return pl.pallas_call(
        functools.partial(table_kernel, spilled, pieces),
        out_shape=jax.ShapeDtypeStruct((block_rows * lines, LANES), jnp.float32),
        in_specs=in_specs,
        out_specs=pl.BlockSpec(memory_space=pl.ANY),
        scratch_shapes=scratch,
        compiler_params=pltpu.CompilerParams(vmem_limit_bytes=VMEM_LIMIT),
    )(*operands)


def on_device(token_ids, embedded, norm_gain, proj_grad, proj_weight, stream_grad):
    n = lax.axis_size("dp")
    tokens = token_ids.shape[1]
    cap = max(2, 2 * tokens // n)
    block_rows = VOCAB // n
    tiers = cap == LANES
    keep = 3 * cap // 8 if tiers else cap
    spill = 9 * cap // 16 if tiers else 0
    rows, index, over, kept = exchange(
        token_ids, embedded[0], norm_gain, proj_grad[0], proj_weight[0], stream_grad[0],
        n, lax.axis_size("mp"), cap, keep, spill, block_rows,
    )
    half = rows.shape[-1]
    if tiers:

        def whole():
            full_rows, full_index = full_exchange(token_ids, kept, n, cap, block_rows)
            return table(full_index, full_rows, None, block_rows)

        def short():
            return table(index, rows, over, block_rows)

        out = lax.cond(jnp.max(index[:, :, 0, index.shape[-1] - LANES]) > 0, whole, short)
    else:
        out = table(index, rows, None, block_rows)
    return out.reshape(block_rows, 1, half)


def solution(mesh):
    return jax.shard_map(
        on_device,
        mesh=mesh,
        in_specs=(
            P("pipe", "dp"),
            P("pipe", "dp", "mp"),
            P("pipe", "mp"),
            P("pipe", "dp", None),
            P("pipe", "mp", None),
            P("pipe", "dp", "mp"),
        ),
        out_specs=P("dp", "mp", "pipe"),
        check_vma=False,
    )
```

```python
import functools

import jax
import jax.numpy as jnp
from jax import lax
from jax.experimental import pallas as pl
from jax.experimental.pallas import tpu as pltpu
from jax.sharding import PartitionSpec as P

VOCAB = 32128
LANES = 128
epsilon = 1e-06
BATCH = 8
VMEM_LIMIT = 60 * 1024 * 1024


def partner(me, k, n):
    out, bit = 0, 1
    while bit < n:
        mine = (me // bit) % 2
        flip = (k // bit) % 2
        out = out + bit * (mine + flip - 2 * mine * flip)
        bit *= 2
    return out


def contract_last(a, b):
    return lax.dot_general(a, b, (((1,), (1,)), ((), ())), preferred_element_type=jnp.float32)


def greet_all(n, pipe, other, me, mp):
    barrier = pltpu.get_barrier_semaphore()

    def greet(k, carry):
        d = partner(me, k, n)
        pl.semaphore_signal(
            barrier, inc=1, device_id={"dp": d, "pipe": other}, device_id_type=pl.DeviceIdType.MESH
        )

        @pl.when(k > 0)
        def _():
            pl.semaphore_signal(
                barrier, inc=1, device_id={"dp": d, "pipe": pipe}, device_id_type=pl.DeviceIdType.MESH
            )

        return carry

    lax.fori_loop(0, n, greet, 0)
    if mp is not None:
        pl.semaphore_signal(
            barrier, inc=1, device_id={"mp": 1 - mp}, device_id_type=pl.DeviceIdType.MESH
        )
    return barrier


def pieces_of(block_rows):
    pieces = 8
    while block_rows % pieces:
        pieces //= 2
    return pieces


def index_lanes(keep):
    return -(-keep // LANES) * LANES


def batches(count):
    return jnp.floor((count + (BATCH - 1)) * (1.0 / BATCH))


def find_places(n, keep, spill, block_rows, me, ids_ref, placer_v, local_v, facts_v):
    tokens = ids_ref.shape[1]
    ids = ids_ref[...].astype(jnp.float32)
    ids_down = jnp.broadcast_to(ids, (LANES, tokens)).T[:, 0:1]
    earlier = lax.broadcasted_iota(jnp.int32, (tokens, tokens), 0) < lax.broadcasted_iota(
        jnp.int32, (tokens, tokens), 1
    )
    same = jnp.where((ids_down == ids) & earlier, 1.0, 0.0)
    first = jnp.where(jnp.sum(same, axis=0, keepdims=True) > 0.0, 0.0, 1.0)
    first_down = jnp.broadcast_to(first, (LANES, tokens)).T[:, 0:1]
    rank = jnp.sum(jnp.where(ids_down < ids, first_down, 0.0), axis=0, keepdims=True)

    k = lax.broadcasted_iota(jnp.int32, (n, 1), 0)
    low = (partner(me, k, n) * block_rows).astype(jnp.float32)

    def below(edge):
        return jnp.sum(jnp.where(ids < edge, first, 0.0), axis=1, keepdims=True)

    pieces = pieces_of(block_rows)
    base = below(low)
    bounds = [below(low + float(q * (block_rows // pieces))) - base for q in range(1, pieces + 1)]
    match = jnp.where((ids >= low) & (ids < low + float(block_rows)), 1.0, 0.0)
    rank = rank - jnp.sum(match * base, axis=0, keepdims=True)
    slot = jnp.sum(match * (k * keep).astype(jnp.float32), axis=0, keepdims=True)
    local = ids - jnp.sum(match * low, axis=0, keepdims=True)
    position = jnp.where(rank < keep, slot + rank, -1.0)
    lane = lax.broadcasted_iota(jnp.int32, (n, LANES), 1)
    facts = jnp.zeros((n, LANES), jnp.float32)
    for q in range(pieces):
        facts = jnp.where(lane == 2 + q, batches(jnp.minimum(bounds[q], keep)), facts)
    if spill:
        over = jnp.maximum(bounds[-1] - keep, 0.0)
        start = jnp.zeros((n, 1), jnp.float32)
        for o in range(n):
            start = start + jnp.where(k > o, over[o:o + 1], 0.0)
        behind = jnp.sum(match * start, axis=0, keepdims=True) + (rank + (n * keep - keep))
        position = jnp.where(rank < keep, position, behind)
        full = jnp.where(jnp.sum(over, axis=0, keepdims=True) > spill, 1.0, 0.0)
        begin = jnp.floor(start * (1.0 / BATCH))
        facts = jnp.where(lane == 0, full, jnp.where(lane == 1, begin, facts))
        for q in range(pieces):
            passed = jnp.maximum(bounds[q] - keep, 0.0)
            passed = jnp.where(passed > 0.0, batches(start + passed), begin)
            facts = jnp.where(lane == 2 + pieces + q, jnp.minimum(passed, float(spill // BATCH)), facts)
    facts_v[...] = facts.astype(jnp.int32)
    high = jnp.floor(local * (1.0 / 64.0))
    row = lax.broadcasted_iota(jnp.int32, (8, tokens), 0)
    parts = jnp.where(row == 0, high, jnp.where(row == 1, local - high * 64.0, 0.0))
    owner = jnp.sum(match * (k + 1).astype(jnp.float32), axis=0, keepdims=True)
    parts = jnp.where(row == 2, owner, parts) * first
    local_v[...] = parts.astype(jnp.bfloat16)
    slots = lax.broadcasted_iota(jnp.int32, placer_v.shape, 0)
    placer_v[...] = jnp.where(position.astype(jnp.int32) == slots, 1.0, 0.0).astype(jnp.bfloat16)


def place_indices(n, keep, spill, block_rows, lines, placer_v, local_v, facts_v, sendi_v):
    parts = contract_last(local_v[...], placer_v[...])
    owner = parts[2:3]
    found = parts[0:1] * 64.0 + parts[1:2]
    found = jnp.where(owner > 0.0, found, float(block_rows))
    found = (found * float(lines)).astype(jnp.int32)
    facts_at = sendi_v.shape[2] - LANES
    sendi_v[...] = jnp.zeros(sendi_v.shape, jnp.int32)
    for k in range(n):
        sendi_v[k, :, 0:keep] = found[:, k * keep:(k + 1) * keep]
        if spill:
            sendi_v[k, :, facts_at - LANES:facts_at] = jnp.where(
                owner[:, n * keep:] == float(k + 1), found[:, n * keep:], block_rows * lines
            )
        sendi_v[k, :, facts_at:] = facts_v[k:k + 1, :]


def place_rows(c, chunk, keep, spill, placer_v, part, send_v, over_v):
    n, _, _, half = send_v.shape
    p, cols = c * chunk // half, pl.ds(c * chunk % half, chunk)
    placed = jnp.dot(
        placer_v[0:n * keep + spill, :], part, preferred_element_type=jnp.float32
    ).astype(jnp.bfloat16)
    send_v[:, p, :, cols] = placed[:n * keep].reshape(n, keep, chunk)
    if spill:
        over_v[p, :, cols] = placed[n * keep:]


def remote(src, dst, send_sem, recv_sem, **where):
    return pltpu.make_async_remote_copy(
        src_ref=src, dst_ref=dst, send_sem=send_sem, recv_sem=recv_sem,
        device_id=where, device_id_type=pl.DeviceIdType.MESH,
    )


def make_sender(n, pipe, other, me, send_v, sendi_v, rows_out, index_out, sems):
    send_sem, recv_sem, isend_sem, irecv_sem = sems

    def copies(k, p, s):
        d = partner(me, k, n)
        return (
            remote(send_v.at[k, p], rows_out.at[k, s], send_sem.at[k, p], recv_sem.at[k, s], dp=d, pipe=p),
            remote(sendi_v.at[k], index_out.at[k, s], isend_sem.at[k, p], irecv_sem.at[k, s], dp=d, pipe=p),
        )

    def send(k, own_chip):
        for copy in copies(k, other, pipe):
            copy.start()
        if not own_chip:
            for copy in copies(k, pipe, pipe):
                copy.start()

    def arrive(k, carry):
        for copy in copies(k, other, pipe):
            copy.wait_send()
        for copy in copies(k, other, other):
            copy.wait_recv()

        @pl.when(k > 0)
        def _():
            for copy in copies(k, pipe, pipe):
                copy.wait_send()
            for copy in copies(k, other, pipe):
                copy.wait_recv()

        return carry

    return send, arrive


def exchange_kernel(
    n, cap, keep, spill, block_rows, full_width, chunk,
    ids_ref, gain_ref, embedded, proj_grad, weight, stream,
    rows_out, index_out, spill_out, kept_out,
    emb_v, grad_v, weight_v, stream_v, scaled_v, rows_v, send_v, sendi_v, over_v, sums_v, sums_got,
    placer_v, local_v, facts_v,
    in_sem, weight_sem, sum_send, sum_recv, send_sem, recv_sem, isend_sem, irecv_sem, own_sem,
    pair_send, pair_recv, line_send, line_recv, side_send, side_recv,
):
    pipe = lax.axis_index("pipe")
    me = lax.axis_index("dp")
    mp = lax.axis_index("mp")
    other = 1 - pipe
    tokens, width = emb_v.shape
    half = width // 2

    loads = [
        pltpu.make_async_copy(proj_grad, grad_v, in_sem.at[0]),
        pltpu.make_async_copy(embedded, emb_v, in_sem.at[1]),
        pltpu.make_async_copy(stream, stream_v, in_sem.at[2]),
    ]
    chunks = [
        pltpu.make_async_copy(
            weight.at[pl.ds(j * chunk, chunk)], weight_v.at[pl.ds(j * chunk, chunk)], weight_sem.at[j]
        )
        for j in range(width // chunk)
    ]
    loads[0].start()
    chunks[0].start()
    barrier = greet_all(n, pipe, other, me, mp)
    find_places(n, keep, spill, block_rows, me, ids_ref, placer_v, local_v, facts_v)
    chunks[1].start()
    loads[1].start()

    loads[0].wait()
    mixed = jnp.zeros((tokens, 1), jnp.float32)
    square = jnp.zeros((tokens, 1), jnp.float32)
    for j in range(width // chunk):
        cols = pl.ds(j * chunk, chunk)
        if j + 2 < width // chunk:
            chunks[j + 2].start()
        else:
            loads[2].start() if j + 2 == width // chunk else None
        chunks[j].wait()
        scaled = contract_last(grad_v[...], weight_v[cols, :]) * gain_ref[:, cols]
        scaled_v[:, cols] = scaled
        if j == 0:
            loads[1].wait()
        inputs = emb_v[:, cols].astype(jnp.float32)
        square = square + jnp.sum(inputs * inputs, axis=1, keepdims=True)
        mixed = mixed + jnp.sum(inputs * scaled, axis=1, keepdims=True)
    lane = lax.broadcasted_iota(jnp.int32, (tokens, LANES), 1)
    packed = jnp.where(lane == 0, square, jnp.where(lane == 1, mixed, 0.0))
    sums_v[...] = packed.T[:8]

    pl.semaphore_wait(barrier, 2 * n)
    swap = remote(sums_v, sums_got, sum_send, sum_recv, mp=1 - mp)
    swap.start()
    place_indices(n, keep, spill, block_rows, half // LANES, placer_v, local_v, facts_v, sendi_v)
    loads[2].wait()
    swap.wait()

    total = sums_v[...] + sums_got[...]
    inverse = lax.rsqrt(total[0:1] / full_width + epsilon)
    coef = inverse * inverse * inverse * total[1:2] / full_width
    line = lax.broadcasted_iota(jnp.int32, (LANES, tokens), 0)
    back = jnp.where(line == 0, inverse, jnp.where(line == 1, coef, 0.0)).T
    for j in range(width // chunk):
        cols = pl.ds(j * chunk, chunk)
        norm_back = back[:, 0:1] * scaled_v[:, cols] - emb_v[:, cols].astype(jnp.float32) * back[:, 1:2]
        part = (stream_v[:, cols].astype(jnp.float32) + norm_back).astype(jnp.bfloat16)
        if spill:
            rows_v[:, cols] = part
        place_rows(j, chunk, keep, spill, placer_v, part, send_v, over_v)

    send, arrive = make_sender(
        n, pipe, other, me, send_v, sendi_v, rows_out, index_out,
        (send_sem, recv_sem, isend_sem, irecv_sem),
    )
    if spill:
        lines = n // 2
        at, beside = me // 2, partner(me, 1, n)
        pair = remote(over_v.at[other], spill_out.at[0, pipe], pair_send, pair_recv, pipe=other)
        pair.start()
        own_over = pltpu.make_async_copy(over_v.at[pipe], spill_out.at[0, pipe], own_sem.at[2])
        own_over.start()
        kept = pltpu.make_async_copy(rows_v, kept_out, own_sem.at[3])
        kept.start()

        def along(up, r, source, to):
            return remote(
                spill_out.at[partner(me, source, n)], spill_out.at[partner(to, source, n)],
                line_send.at[up, r], line_recv.at[up, r], dp=to,
            )

        def across(source):
            return remote(
                spill_out.at[partner(me, source, n)], spill_out.at[partner(beside, source, n)],
                side_send.at[source // 2], side_recv.at[source // 2], dp=beside,
            )

        def pass_on(r):
            for up in (1, 0):
                step = 2 if up else -2
                source = me - step * r
                here = (at >= r) if up else (at + r < lines)
                more = (at + 1 < lines) if up else (at >= 1)
                if r > 0:

                    @pl.when(here)
                    def _():
                        remote(
                            spill_out.at[0], spill_out.at[partner(me, source, n)],
                            line_send.at[up, r], line_recv.at[up, r], dp=beside,
                        ).wait_recv()
                        across(source).start()

                @pl.when(here & more)
                def _():
                    along(up, r + 1, source, me + step).start()

            if r == 0:
                across(me).start()

        def finish(r):
            for up in (1, 0):
                step = 2 if up else -2
                source = me - step * r
                here = (at >= r) if up else (at + r < lines)
                more = (at + 1 < lines) if up else (at >= 1)

                @pl.when(here & more)
                def _():
                    along(up, r + 1, source, me + step).wait_send()

        send(1, False)
        own_over.wait()
        pair.wait()
        pass_on(0)
        for k in range(2, n):
            send(k, False)
            if k % 2 == 1 and k // 2 < lines:
                pass_on(k // 2)
        send(0, True)
    else:

        def send_on(k, carry):
            send(k, False)
            return carry

        lax.fori_loop(1, n, send_on, 0)
        send(0, True)
    own_rows = pltpu.make_async_copy(send_v.at[0, pipe], rows_out.at[0, pipe], own_sem.at[0])
    own_index = pltpu.make_async_copy(sendi_v.at[0], index_out.at[0, pipe], own_sem.at[1])
    own_rows.start()
    own_index.start()
    lax.fori_loop(0, n, arrive, 0)
    own_rows.wait()
    own_index.wait()
    if spill:
        for r in range(lines):
            finish(r)

        def side(z, carry):
            remote(
                spill_out.at[partner(me, 2 * z, n)], spill_out.at[partner(me, 2 * z + beside % 2, n)],
                side_send.at[z], side_recv.at[z], dp=beside,
            ).wait()
            return carry

        lax.fori_loop(0, lines, side, 0)
        kept.wait()


def exchange(ids, embedded, gain, proj_grad, weight, stream, n, n_mp, cap, keep, spill, block_rows):
    tokens, width = embedded.shape
    inner = proj_grad.shape[1]
    half = width // 2
    chunk = min(512, half)
    index_width = index_lanes(keep) + (2 * LANES if spill else LANES)
    over = (spill or 16, half)
    kept = (tokens, width) if spill else (8, LANES)
    any_space = pl.BlockSpec(memory_space=pl.ANY)
    vmem = pl.BlockSpec(memory_space=pltpu.VMEM)
    dma = pltpu.SemaphoreType.DMA
    return pl.pallas_call(
        functools.partial(exchange_kernel, n, cap, keep, spill, block_rows, width * n_mp, chunk),
        out_shape=(
            jax.ShapeDtypeStruct((n, 2, keep, half), jnp.bfloat16),
            jax.ShapeDtypeStruct((n, 2, 1, index_width), jnp.int32),
            jax.ShapeDtypeStruct((n if spill else 1, 2) + over, jnp.bfloat16),
            jax.ShapeDtypeStruct(kept, jnp.bfloat16),
        ),
        in_specs=[vmem, vmem] + [any_space] * 4,
        out_specs=(any_space,) * 4,
        scratch_shapes=[
            pltpu.VMEM((tokens, width), jnp.bfloat16),
            pltpu.VMEM((tokens, inner), jnp.bfloat16),
            pltpu.VMEM((width, inner), jnp.bfloat16),
            pltpu.VMEM((tokens, width), jnp.bfloat16),
            pltpu.VMEM((tokens, width), jnp.float32),
            pltpu.VMEM((tokens, width), jnp.bfloat16),
            pltpu.VMEM((n, 2, keep, half), jnp.bfloat16),
            pltpu.VMEM((n, 1, index_width), jnp.int32),
            pltpu.VMEM((2,) + over, jnp.bfloat16),
            pltpu.VMEM((8, tokens), jnp.float32),
            pltpu.VMEM((8, tokens), jnp.float32),
            pltpu.VMEM((n * keep + (LANES if spill else 0), tokens), jnp.bfloat16),
            pltpu.VMEM((8, tokens), jnp.bfloat16),
            pltpu.VMEM((n, LANES), jnp.int32),
            dma((3,)),
            dma((width // chunk,)),
            dma,
            dma,
            dma((n, 2)),
            dma((n, 2)),
            dma((n, 2)),
            dma((n, 2)),
            dma((4,)),
            dma,
            dma,
            dma((2, n)),
            dma((2, n)),
            dma((n,)),
            dma((n,)),
        ],
        compiler_params=pltpu.CompilerParams(
            collective_id=0, has_side_effects=True, vmem_limit_bytes=VMEM_LIMIT
        ),
    )(ids, gain, embedded, proj_grad, weight, stream)


def full_kernel(
    n, cap, block_rows, ids_ref, rows_v, rows_out, index_out, send_v, sendi_v, placer_v, local_v, facts_v,
    send_sem, recv_sem, isend_sem, irecv_sem, own_sem,
):
    pipe = lax.axis_index("pipe")
    me = lax.axis_index("dp")
    other = 1 - pipe
    barrier = greet_all(n, pipe, other, me, None)
    pl.semaphore_wait(barrier, 2 * n - 1)
    find_places(n, cap, 0, block_rows, me, ids_ref, placer_v, local_v, facts_v)
    width = rows_v.shape[1]
    place_indices(n, cap, 0, block_rows, width // 2 // LANES, placer_v, local_v, facts_v, sendi_v)
    chunk = min(256, width // 2)
    for c in range(width // chunk):
        place_rows(c, chunk, cap, 0, placer_v, rows_v[:, c * chunk:(c + 1) * chunk], send_v, None)
    send, arrive = make_sender(
        n, pipe, other, me, send_v, sendi_v, rows_out, index_out,
        (send_sem, recv_sem, isend_sem, irecv_sem),
    )

    def send_on(k, carry):
        send(k, False)
        return carry

    lax.fori_loop(1, n, send_on, 0)
    send(0, True)
    own_rows = pltpu.make_async_copy(send_v.at[0, pipe], rows_out.at[0, pipe], own_sem.at[0])
    own_index = pltpu.make_async_copy(sendi_v.at[0], index_out.at[0, pipe], own_sem.at[1])
    own_rows.start()
    own_index.start()
    lax.fori_loop(0, n, arrive, 0)
    own_rows.wait()
    own_index.wait()


def full_exchange(ids, rows, n, cap, block_rows):
    tokens, width = rows.shape
    half = width // 2
    any_space = pl.BlockSpec(memory_space=pl.ANY)
    vmem = pl.BlockSpec(memory_space=pltpu.VMEM)
    dma = pltpu.SemaphoreType.DMA
    return pl.pallas_call(
        functools.partial(full_kernel, n, cap, block_rows),
        out_shape=(
            jax.ShapeDtypeStruct((n, 2, cap, half), jnp.bfloat16),
            jax.ShapeDtypeStruct((n, 2, 1, index_lanes(cap) + LANES), jnp.int32),
        ),
        in_specs=[vmem, vmem],
        out_specs=(any_space, any_space),
        scratch_shapes=[
            pltpu.VMEM((n, 2, cap, half), jnp.bfloat16),
            pltpu.VMEM((n, 1, index_lanes(cap) + LANES), jnp.int32),
            pltpu.VMEM((n * cap, tokens), jnp.bfloat16),
            pltpu.VMEM((8, tokens), jnp.bfloat16),
            pltpu.VMEM((n, LANES), jnp.int32),
            dma((n, 2)),
            dma((n, 2)),
            dma((n, 2)),
            dma((n, 2)),
            dma((2,)),
        ],
        compiler_params=pltpu.CompilerParams(
            collective_id=1, has_side_effects=True, vmem_limit_bytes=VMEM_LIMIT
        ),
    )(ids, rows)


def table_kernel(spilled, width, pieces, index_ref, rows_ref, *rest):
    if spilled:
        over_ref, out_ref, rows_v, wide_v, over_v, table_v, sem, in_sem = rest
    else:
        out_ref, rows_v, wide_v, table_v, sem, in_sem = rest
    blocks, keep, half = rows_ref.shape
    load = pltpu.make_async_copy(rows_ref, rows_v, in_sem)
    load.start()
    lines = half // LANES
    span = out_ref.shape[0] // pieces
    facts_at = width - LANES
    parts = 16
    while out_ref.shape[0] % (8 * parts):
        parts //= 2
    clear_rows = out_ref.shape[0] // parts

    def clear(i, carry):
        table_v[pl.ds(pl.multiple_of(i * clear_rows, 8), clear_rows), :] = jnp.zeros(
            (clear_rows, LANES), jnp.float32
        )
        return carry

    lax.fori_loop(0, parts, clear, 0)
    load.wait()

    def widen(b, carry):
        for j in range(lines):
            wide_v[pl.ds(b * keep * lines + j, keep, stride=lines), :] = rows_v[
                b, :, j * LANES:(j + 1) * LANES
            ].astype(jnp.float32)
        if spilled:

            @pl.when(index_ref[b * width + facts_at + 1 + 2 * pieces] > index_ref[b * width + facts_at + 1])
            def _():
                for j in range(lines):
                    over_v[pl.ds(b * spilled * lines + j, spilled, stride=lines), :] = over_ref[
                        b, :, j * LANES:(j + 1) * LANES
                    ].astype(jnp.float32)

        return carry

    lax.fori_loop(0, blocks, widen, 0)

    def add_rows(source_v, b, size, index_from, start, stop):
        def add(g, carry):
            first = g * BATCH
            place = pl.multiple_of((b * size + first) * lines, BATCH * lines)
            places = [
                pl.multiple_of(index_ref[b * width + index_from + first + u], lines) for u in range(BATCH)
            ]
            sums = [
                table_v[pl.ds(places[u], lines), :] + source_v[pl.ds(place + u * lines, lines), :]
                for u in range(BATCH)
            ]
            for u in range(BATCH):
                table_v[pl.ds(places[u], lines), :] = sums[u]
            return carry

        lax.fori_loop(start, stop, add, 0)

    copies = []
    for q in range(pieces):

        def block(b, carry):
            start = index_ref[b * width + facts_at + 1 + q] if q else 0
            add_rows(wide_v, b, keep, 0, start, index_ref[b * width + facts_at + 2 + q])
            if spilled:
                start = index_ref[b * width + facts_at + (1 + pieces + q if q else 1)]
                add_rows(
                    over_v, b, spilled, facts_at - LANES, start,
                    index_ref[b * width + facts_at + 2 + pieces + q],
                )
            return carry

        lax.fori_loop(0, blocks, block, 0)
        rows = pl.ds(q * span, span)
        copies.append(pltpu.make_async_copy(table_v.at[rows], out_ref.at[rows], sem.at[q]))
        copies[q].start()
    for copy in copies:
        copy.wait()


def table(index, rows, over, block_rows):
    n, stacks, keep, half = rows.shape
    lines = half // LANES
    blocks = n * stacks
    pieces = pieces_of(block_rows)
    spilled = 0 if over is None else over.shape[2]
    vmem = pl.BlockSpec(memory_space=pltpu.VMEM)
    operands = [index.reshape(-1), rows.reshape(blocks, keep, half)]
    any_space = pl.BlockSpec(memory_space=pl.ANY)
    in_specs = [pl.BlockSpec(memory_space=pltpu.SMEM), any_space]
    scratch = [pltpu.VMEM((blocks, keep, half), jnp.bfloat16)]
    scratch += [pltpu.VMEM((blocks * keep * lines, LANES), jnp.float32)]
    if spilled:
        operands.append(over.reshape(blocks, spilled, half))
        in_specs.append(vmem)
        scratch.append(pltpu.VMEM((blocks * spilled * lines, LANES), jnp.float32))
    scratch.append(pltpu.VMEM(((block_rows + 1) * lines, LANES), jnp.float32))
    scratch += [pltpu.SemaphoreType.DMA((pieces,)), pltpu.SemaphoreType.DMA]
    return pl.pallas_call(
        functools.partial(table_kernel, spilled, index.shape[-1], pieces),
        out_shape=jax.ShapeDtypeStruct((block_rows * lines, LANES), jnp.float32),
        in_specs=in_specs,
        out_specs=any_space,
        scratch_shapes=scratch,
        compiler_params=pltpu.CompilerParams(vmem_limit_bytes=VMEM_LIMIT),
    )(*operands)


def on_device(token_ids, embedded, norm_gain, proj_grad, proj_weight, stream_grad):
    n = lax.axis_size("dp")
    tokens = token_ids.shape[1]
    cap = max(2, 2 * tokens // n)
    block_rows = VOCAB // n
    tiers = cap == LANES
    keep = 3 * cap // 8 if tiers else cap
    spill = 9 * cap // 16 if tiers else 0
    rows, index, over, kept = exchange(
        token_ids, embedded[0], norm_gain, proj_grad[0], proj_weight[0], stream_grad[0],
        n, lax.axis_size("mp"), cap, keep, spill, block_rows,
    )
    half = rows.shape[-1]
    if tiers:

        def whole():
            full_rows, full_index = full_exchange(token_ids, kept, n, cap, block_rows)
            return table(full_index, full_rows, None, block_rows)

        def short():
            return table(index, rows, over, block_rows)

        out = lax.cond(jnp.max(index[:, :, 0, index.shape[-1] - LANES]) > 0, whole, short)
    else:
        out = table(index, rows, None, block_rows)
    return out.reshape(block_rows, 1, half)


def solution(mesh):
    return jax.shard_map(
        on_device,
        mesh=mesh,
        in_specs=(
            P("pipe", "dp"),
            P("pipe", "dp", "mp"),
            P("pipe", "mp"),
            P("pipe", "dp", None),
            P("pipe", "mp", None),
            P("pipe", "dp", "mp"),
        ),
        out_specs=P("dp", "mp", "pipe"),
        check_vma=False,
    )
```

```python
import functools

import jax
import jax.numpy as jnp
from jax import lax
from jax.experimental import pallas as pl
from jax.experimental.pallas import tpu as pltpu
from jax.sharding import PartitionSpec as P

VOCAB = 32128
LANES = 128
epsilon = 1e-06
BATCH = 8
VMEM_LIMIT = 60 * 1024 * 1024


def partner(me, k, n):
    out, bit = 0, 1
    while bit < n:
        mine = (me // bit) % 2
        flip = (k // bit) % 2
        out = out + bit * (mine + flip - 2 * mine * flip)
        bit *= 2
    return out


def contract_last(a, b):
    return lax.dot_general(a, b, (((1,), (1,)), ((), ())), preferred_element_type=jnp.float32)


def greet_all(n, pipe, other, me, mp):
    barrier = pltpu.get_barrier_semaphore()

    def greet(k, carry):
        d = partner(me, k, n)
        pl.semaphore_signal(
            barrier, inc=1, device_id={"dp": d, "pipe": other}, device_id_type=pl.DeviceIdType.MESH
        )

        @pl.when(k > 0)
        def _():
            pl.semaphore_signal(
                barrier, inc=1, device_id={"dp": d, "pipe": pipe}, device_id_type=pl.DeviceIdType.MESH
            )

        return carry

    lax.fori_loop(0, n, greet, 0)
    if mp is not None:
        pl.semaphore_signal(
            barrier, inc=1, device_id={"mp": 1 - mp}, device_id_type=pl.DeviceIdType.MESH
        )
    return barrier


def pieces_of(block_rows):
    pieces = 8
    while block_rows % pieces:
        pieces //= 2
    return pieces


def index_lanes(keep):
    return -(-keep // LANES) * LANES


def batches(count):
    return jnp.floor((count + (BATCH - 1)) * (1.0 / BATCH))


def find_places(n, keep, spill, block_rows, me, ids_ref, placer_v, local_v, facts_v):
    tokens = ids_ref.shape[1]
    ids = ids_ref[...].astype(jnp.float32)
    ids_down = jnp.broadcast_to(ids, (LANES, tokens)).T[:, 0:1]
    earlier = lax.broadcasted_iota(jnp.int32, (tokens, tokens), 0) < lax.broadcasted_iota(
        jnp.int32, (tokens, tokens), 1
    )
    same = jnp.where((ids_down == ids) & earlier, 1.0, 0.0)
    first = jnp.where(jnp.sum(same, axis=0, keepdims=True) > 0.0, 0.0, 1.0)
    first_down = jnp.broadcast_to(first, (LANES, tokens)).T[:, 0:1]
    rank = jnp.sum(jnp.where(ids_down < ids, first_down, 0.0), axis=0, keepdims=True)

    k = lax.broadcasted_iota(jnp.int32, (n, 1), 0)
    low = (partner(me, k, n) * block_rows).astype(jnp.float32)

    def below(edge):
        return jnp.sum(jnp.where(ids < edge, first, 0.0), axis=1, keepdims=True)

    pieces = pieces_of(block_rows)
    base = below(low)
    bounds = [below(low + float(q * (block_rows // pieces))) - base for q in range(1, pieces + 1)]
    match = jnp.where((ids >= low) & (ids < low + float(block_rows)), 1.0, 0.0)
    rank = rank - jnp.sum(match * base, axis=0, keepdims=True)
    slot = jnp.sum(match * (k * keep).astype(jnp.float32), axis=0, keepdims=True)
    local = ids - jnp.sum(match * low, axis=0, keepdims=True)
    position = jnp.where(rank < keep, slot + rank, -1.0)
    lane = lax.broadcasted_iota(jnp.int32, (n, LANES), 1)
    facts = jnp.zeros((n, LANES), jnp.float32)
    for q in range(pieces):
        facts = jnp.where(lane == 2 + q, batches(jnp.minimum(bounds[q], keep)), facts)
    if spill:
        over = jnp.maximum(bounds[-1] - keep, 0.0)
        start = jnp.zeros((n, 1), jnp.float32)
        for o in range(n):
            start = start + jnp.where(k > o, over[o:o + 1], 0.0)
        behind = jnp.sum(match * start, axis=0, keepdims=True) + (rank + (n * keep - keep))
        position = jnp.where(rank < keep, position, behind)
        full = jnp.where(jnp.sum(over, axis=0, keepdims=True) > spill, 1.0, 0.0)
        begin = jnp.floor(start * (1.0 / BATCH))
        facts = jnp.where(lane == 0, full, jnp.where(lane == 1, begin, facts))
        for q in range(pieces):
            passed = jnp.maximum(bounds[q] - keep, 0.0)
            passed = jnp.where(passed > 0.0, batches(start + passed), begin)
            facts = jnp.where(lane == 2 + pieces + q, jnp.minimum(passed, float(spill // BATCH)), facts)
    facts_v[...] = facts.astype(jnp.int32)
    high = jnp.floor(local * (1.0 / 64.0))
    row = lax.broadcasted_iota(jnp.int32, (8, tokens), 0)
    parts = jnp.where(row == 0, high, jnp.where(row == 1, local - high * 64.0, 0.0))
    owner = jnp.sum(match * (k + 1).astype(jnp.float32), axis=0, keepdims=True)
    parts = jnp.where(row == 2, owner, parts) * first
    local_v[...] = parts.astype(jnp.bfloat16)
    slots = lax.broadcasted_iota(jnp.int32, placer_v.shape, 0)
    placer_v[...] = jnp.where(position.astype(jnp.int32) == slots, 1.0, 0.0).astype(jnp.bfloat16)


def place_indices(n, keep, spill, block_rows, lines, placer_v, local_v, facts_v, sendi_v):
    parts = contract_last(local_v[...], placer_v[...])
    owner = parts[2:3]
    found = parts[0:1] * 64.0 + parts[1:2]
    found = jnp.where(owner > 0.0, found, float(block_rows))
    found = (found * float(lines)).astype(jnp.int32)
    facts_at = sendi_v.shape[2] - LANES
    sendi_v[...] = jnp.zeros(sendi_v.shape, jnp.int32)
    for k in range(n):
        sendi_v[k, :, 0:keep] = found[:, k * keep:(k + 1) * keep]
        if spill:
            sendi_v[k, :, facts_at - LANES:facts_at] = jnp.where(
                owner[:, n * keep:] == float(k + 1), found[:, n * keep:], block_rows * lines
            )
        sendi_v[k, :, facts_at:] = facts_v[k:k + 1, :]


def place_rows(p, first, chunk, keep, spill, placer_v, part, send_v, over_v):
    n = send_v.shape[0]
    cols = pl.ds(first, chunk)
    placed = jnp.dot(
        placer_v[0:n * keep + spill, :], part, preferred_element_type=jnp.float32
    ).astype(jnp.bfloat16)
    send_v[:, p, :, cols] = placed[:n * keep].reshape(n, keep, chunk)
    if spill:
        over_v[p, :, cols] = placed[n * keep:]


def remote(src, dst, send_sem, recv_sem, **where):
    return pltpu.make_async_remote_copy(
        src_ref=src, dst_ref=dst, send_sem=send_sem, recv_sem=recv_sem,
        device_id=where, device_id_type=pl.DeviceIdType.MESH,
    )


def make_sender(n, pipe, other, me, send_v, sendi_v, rows_out, index_out, sems):
    send_sem, recv_sem, isend_sem, irecv_sem = sems

    def copies(k, p, s):
        d = partner(me, k, n)
        return (
            remote(send_v.at[k, p], rows_out.at[k, s], send_sem.at[k, p], recv_sem.at[k, s], dp=d, pipe=p),
            remote(sendi_v.at[k], index_out.at[k, s], isend_sem.at[k, p], irecv_sem.at[k, s], dp=d, pipe=p),
        )

    def send(k, own_chip):
        copies(k, other, pipe)[0].start()
        if not own_chip:
            copies(k, pipe, pipe)[0].start()

    def send_indices():
        def send_index(k, carry):
            copies(k, other, pipe)[1].start()
            copies(k, pipe, pipe)[1].start()
            return carry

        lax.fori_loop(1, n, send_index, 0)
        copies(0, other, pipe)[1].start()

    def arrive(k, carry):
        for copy in copies(k, other, pipe):
            copy.wait_send()
        for copy in copies(k, other, other):
            copy.wait_recv()

        @pl.when(k > 0)
        def _():
            for copy in copies(k, pipe, pipe):
                copy.wait_send()
            for copy in copies(k, other, pipe):
                copy.wait_recv()

        return carry

    return send_indices, send, arrive


def exchange_kernel(
    n, cap, keep, spill, block_rows, full_width, chunk,
    ids_ref, gain_ref, embedded, proj_grad, weight, stream,
    rows_out, index_out, spill_out, kept_out,
    emb_v, grad_v, weight_v, stream_v, scaled_v, rows_v, send_v, sendi_v, over_v, sums_v, sums_got,
    placer_v, local_v, facts_v,
    in_sem, weight_sem, sum_send, sum_recv, send_sem, recv_sem, isend_sem, irecv_sem, own_sem,
    pair_send, pair_recv, line_send, line_recv, side_send, side_recv,
):
    pipe = lax.axis_index("pipe")
    me = lax.axis_index("dp")
    mp = lax.axis_index("mp")
    other = 1 - pipe
    tokens, width = emb_v.shape
    half = width // 2

    loads = [
        pltpu.make_async_copy(proj_grad, grad_v, in_sem.at[0]),
        pltpu.make_async_copy(embedded, emb_v, in_sem.at[1]),
        pltpu.make_async_copy(stream, stream_v, in_sem.at[2]),
    ]
    chunks = [
        pltpu.make_async_copy(
            weight.at[pl.ds(j * chunk, chunk)], weight_v.at[pl.ds(j * chunk, chunk)], weight_sem.at[j]
        )
        for j in range(width // chunk)
    ]
    loads[0].start()
    chunks[0].start()
    barrier = greet_all(n, pipe, other, me, mp)
    find_places(n, keep, spill, block_rows, me, ids_ref, placer_v, local_v, facts_v)
    chunks[1].start()
    loads[1].start()

    loads[0].wait()
    mixed = jnp.zeros((tokens, 1), jnp.float32)
    square = jnp.zeros((tokens, 1), jnp.float32)
    for j in range(width // chunk):
        cols = pl.ds(j * chunk, chunk)
        if j + 2 < width // chunk:
            chunks[j + 2].start()
        else:
            loads[2].start() if j + 2 == width // chunk else None
        chunks[j].wait()
        scaled = contract_last(grad_v[...], weight_v[cols, :]) * gain_ref[:, cols]
        scaled_v[:, cols] = scaled
        if j == 0:
            loads[1].wait()
        inputs = emb_v[:, cols].astype(jnp.float32)
        square = square + jnp.sum(inputs * inputs, axis=1, keepdims=True)
        mixed = mixed + jnp.sum(inputs * scaled, axis=1, keepdims=True)
    lane = lax.broadcasted_iota(jnp.int32, (tokens, LANES), 1)
    packed = jnp.where(lane == 0, square, jnp.where(lane == 1, mixed, 0.0))
    sums_v[...] = packed.T[:8]

    pl.semaphore_wait(barrier, 2 * n)
    swap = remote(sums_v, sums_got, sum_send, sum_recv, mp=1 - mp)
    swap.start()
    place_indices(n, keep, spill, block_rows, half // LANES, placer_v, local_v, facts_v, sendi_v)
    send_indices, send, arrive = make_sender(
        n, pipe, other, me, send_v, sendi_v, rows_out, index_out,
        (send_sem, recv_sem, isend_sem, irecv_sem),
    )
    send_indices()
    loads[2].wait()
    swap.wait()

    total = sums_v[...] + sums_got[...]
    inverse = lax.rsqrt(total[0:1] / full_width + epsilon)
    coef = inverse * inverse * inverse * total[1:2] / full_width
    line = lax.broadcasted_iota(jnp.int32, (LANES, tokens), 0)
    back = jnp.where(line == 0, inverse, jnp.where(line == 1, coef, 0.0)).T
    if spill:
        pair = remote(over_v.at[other], spill_out.at[0, pipe], pair_send, pair_recv, pipe=other)
    for h in range(2):
        p = pipe if h else other
        for first in range(0, half, chunk):
            cols = pl.ds(pl.multiple_of(p * half + first, chunk), chunk)
            norm_back = back[:, 0:1] * scaled_v[:, cols] - emb_v[:, cols].astype(jnp.float32) * back[:, 1:2]
            part = (stream_v[:, cols].astype(jnp.float32) + norm_back).astype(jnp.bfloat16)
            if spill:
                rows_v[:, cols] = part
            place_rows(p, first, chunk, keep, spill, placer_v, part, send_v, over_v)
        if spill and h == 0:
            pair.start()

    if spill:
        lines = n // 2
        at, beside = me // 2, partner(me, 1, n)
        own_over = pltpu.make_async_copy(over_v.at[pipe], spill_out.at[0, pipe], own_sem.at[2])
        own_over.start()
        kept = pltpu.make_async_copy(rows_v, kept_out, own_sem.at[3])
        kept.start()

        def along(up, r, source, to):
            return remote(
                spill_out.at[partner(me, source, n)], spill_out.at[partner(to, source, n)],
                line_send.at[up, r], line_recv.at[up, r], dp=to,
            )

        def across(source):
            return remote(
                spill_out.at[partner(me, source, n)], spill_out.at[partner(beside, source, n)],
                side_send.at[source // 2], side_recv.at[source // 2], dp=beside,
            )

        def pass_on(r):
            for up in (1, 0):
                step = 2 if up else -2
                source = me - step * r
                here = (at >= r) if up else (at + r < lines)
                more = (at + 1 < lines) if up else (at >= 1)
                if r > 0:

                    @pl.when(here)
                    def _():
                        remote(
                            spill_out.at[0], spill_out.at[partner(me, source, n)],
                            line_send.at[up, r], line_recv.at[up, r], dp=beside,
                        ).wait_recv()
                        across(source).start()

                @pl.when(here & more)
                def _():
                    along(up, r + 1, source, me + step).start()

            if r == 0:
                across(me).start()

        def finish(r):
            for up in (1, 0):
                step = 2 if up else -2
                source = me - step * r
                here = (at >= r) if up else (at + r < lines)
                more = (at + 1 < lines) if up else (at >= 1)

                @pl.when(here & more)
                def _():
                    along(up, r + 1, source, me + step).wait_send()

        send(1, False)
        own_over.wait()
        pair.wait()
        pass_on(0)
        for k in range(2, n):
            send(k, False)
            if k % 2 == 1 and k // 2 < lines:
                pass_on(k // 2)
        send(0, True)
    else:

        def send_on(k, carry):
            send(k, False)
            return carry

        lax.fori_loop(1, n, send_on, 0)
        send(0, True)
    own_rows = pltpu.make_async_copy(send_v.at[0, pipe], rows_out.at[0, pipe], own_sem.at[0])
    own_index = pltpu.make_async_copy(sendi_v.at[0], index_out.at[0, pipe], own_sem.at[1])
    own_rows.start()
    own_index.start()
    lax.fori_loop(0, n, arrive, 0)
    own_rows.wait()
    own_index.wait()
    if spill:
        for r in range(lines):
            finish(r)

        def side(z, carry):
            remote(
                spill_out.at[partner(me, 2 * z, n)], spill_out.at[partner(me, 2 * z + beside % 2, n)],
                side_send.at[z], side_recv.at[z], dp=beside,
            ).wait()
            return carry

        lax.fori_loop(0, lines, side, 0)
        kept.wait()


def exchange(ids, embedded, gain, proj_grad, weight, stream, n, n_mp, cap, keep, spill, block_rows):
    tokens, width = embedded.shape
    inner = proj_grad.shape[1]
    half = width // 2
    chunk = min(512, half)
    index_width = index_lanes(keep) + (2 * LANES if spill else LANES)
    over = (spill or 16, half)
    kept = (tokens, width) if spill else (8, LANES)
    any_space = pl.BlockSpec(memory_space=pl.ANY)
    vmem = pl.BlockSpec(memory_space=pltpu.VMEM)
    dma = pltpu.SemaphoreType.DMA
    return pl.pallas_call(
        functools.partial(exchange_kernel, n, cap, keep, spill, block_rows, width * n_mp, chunk),
        out_shape=(
            jax.ShapeDtypeStruct((n, 2, keep, half), jnp.bfloat16),
            jax.ShapeDtypeStruct((n, 2, 1, index_width), jnp.int32),
            jax.ShapeDtypeStruct((n if spill else 1, 2) + over, jnp.bfloat16),
            jax.ShapeDtypeStruct(kept, jnp.bfloat16),
        ),
        in_specs=[vmem, vmem] + [any_space] * 4,
        out_specs=(any_space,) * 4,
        scratch_shapes=[
            pltpu.VMEM((tokens, width), jnp.bfloat16),
            pltpu.VMEM((tokens, inner), jnp.bfloat16),
            pltpu.VMEM((width, inner), jnp.bfloat16),
            pltpu.VMEM((tokens, width), jnp.bfloat16),
            pltpu.VMEM((tokens, width), jnp.float32),
            pltpu.VMEM((tokens, width), jnp.bfloat16),
            pltpu.VMEM((n, 2, keep, half), jnp.bfloat16),
            pltpu.VMEM((n, 1, index_width), jnp.int32),
            pltpu.VMEM((2,) + over, jnp.bfloat16),
            pltpu.VMEM((8, tokens), jnp.float32),
            pltpu.VMEM((8, tokens), jnp.float32),
            pltpu.VMEM((n * keep + (LANES if spill else 0), tokens), jnp.bfloat16),
            pltpu.VMEM((8, tokens), jnp.bfloat16),
            pltpu.VMEM((n, LANES), jnp.int32),
            dma((3,)),
            dma((width // chunk,)),
            dma,
            dma,
            dma((n, 2)),
            dma((n, 2)),
            dma((n, 2)),
            dma((n, 2)),
            dma((4,)),
            dma,
            dma,
            dma((2, n)),
            dma((2, n)),
            dma((n,)),
            dma((n,)),
        ],
        compiler_params=pltpu.CompilerParams(
            collective_id=0, has_side_effects=True, vmem_limit_bytes=VMEM_LIMIT
        ),
    )(ids, gain, embedded, proj_grad, weight, stream)


def full_kernel(
    n, cap, block_rows, ids_ref, rows_v, rows_out, index_out, send_v, sendi_v, placer_v, local_v, facts_v,
    send_sem, recv_sem, isend_sem, irecv_sem, own_sem,
):
    pipe = lax.axis_index("pipe")
    me = lax.axis_index("dp")
    other = 1 - pipe
    barrier = greet_all(n, pipe, other, me, None)
    pl.semaphore_wait(barrier, 2 * n - 1)
    find_places(n, cap, 0, block_rows, me, ids_ref, placer_v, local_v, facts_v)
    width = rows_v.shape[1]
    place_indices(n, cap, 0, block_rows, width // 2 // LANES, placer_v, local_v, facts_v, sendi_v)
    chunk = min(256, width // 2)
    for c in range(width // chunk):
        place_rows(
            c * chunk // (width // 2), c * chunk % (width // 2), chunk, cap, 0, placer_v,
            rows_v[:, c * chunk:(c + 1) * chunk], send_v, None,
        )
    send_indices, send, arrive = make_sender(
        n, pipe, other, me, send_v, sendi_v, rows_out, index_out,
        (send_sem, recv_sem, isend_sem, irecv_sem),
    )
    send_indices()

    def send_on(k, carry):
        send(k, False)
        return carry

    lax.fori_loop(1, n, send_on, 0)
    send(0, True)
    own_rows = pltpu.make_async_copy(send_v.at[0, pipe], rows_out.at[0, pipe], own_sem.at[0])
    own_index = pltpu.make_async_copy(sendi_v.at[0], index_out.at[0, pipe], own_sem.at[1])
    own_rows.start()
    own_index.start()
    lax.fori_loop(0, n, arrive, 0)
    own_rows.wait()
    own_index.wait()


def full_exchange(ids, rows, n, cap, block_rows):
    tokens, width = rows.shape
    half = width // 2
    any_space = pl.BlockSpec(memory_space=pl.ANY)
    vmem = pl.BlockSpec(memory_space=pltpu.VMEM)
    dma = pltpu.SemaphoreType.DMA
    return pl.pallas_call(
        functools.partial(full_kernel, n, cap, block_rows),
        out_shape=(
            jax.ShapeDtypeStruct((n, 2, cap, half), jnp.bfloat16),
            jax.ShapeDtypeStruct((n, 2, 1, index_lanes(cap) + LANES), jnp.int32),
        ),
        in_specs=[vmem, vmem],
        out_specs=(any_space, any_space),
        scratch_shapes=[
            pltpu.VMEM((n, 2, cap, half), jnp.bfloat16),
            pltpu.VMEM((n, 1, index_lanes(cap) + LANES), jnp.int32),
            pltpu.VMEM((n * cap, tokens), jnp.bfloat16),
            pltpu.VMEM((8, tokens), jnp.bfloat16),
            pltpu.VMEM((n, LANES), jnp.int32),
            dma((n, 2)),
            dma((n, 2)),
            dma((n, 2)),
            dma((n, 2)),
            dma((2,)),
        ],
        compiler_params=pltpu.CompilerParams(
            collective_id=1, has_side_effects=True, vmem_limit_bytes=VMEM_LIMIT
        ),
    )(ids, rows)


def table_kernel(spilled, width, pieces, index_ref, rows_ref, *rest):
    if spilled:
        over_ref, out_ref, rows_v, wide_v, over_v, table_v, sem, in_sem = rest
    else:
        out_ref, rows_v, wide_v, table_v, sem, in_sem = rest
    blocks, keep, half = rows_ref.shape
    load = pltpu.make_async_copy(rows_ref, rows_v, in_sem)
    load.start()
    lines = half // LANES
    span = out_ref.shape[0] // pieces
    facts_at = width - LANES
    parts = 16
    while out_ref.shape[0] % (8 * parts):
        parts //= 2
    clear_rows = out_ref.shape[0] // parts

    def clear(i, carry):
        table_v[pl.ds(pl.multiple_of(i * clear_rows, 8), clear_rows), :] = jnp.zeros(
            (clear_rows, LANES), jnp.float32
        )
        return carry

    lax.fori_loop(0, parts, clear, 0)
    load.wait()

    def widen(b, carry):
        for j in range(lines):
            wide_v[pl.ds(b * keep * lines + j, keep, stride=lines), :] = rows_v[
                b, :, j * LANES:(j + 1) * LANES
            ].astype(jnp.float32)
        if spilled:

            @pl.when(index_ref[b * width + facts_at + 1 + 2 * pieces] > index_ref[b * width + facts_at + 1])
            def _():
                for j in range(lines):
                    over_v[pl.ds(b * spilled * lines + j, spilled, stride=lines), :] = over_ref[
                        b, :, j * LANES:(j + 1) * LANES
                    ].astype(jnp.float32)

        return carry

    lax.fori_loop(0, blocks, widen, 0)

    def add_rows(source_v, b, size, index_from, start, stop):
        def add(g, carry):
            first = g * BATCH
            place = pl.multiple_of((b * size + first) * lines, BATCH * lines)
            places = [
                pl.multiple_of(index_ref[b * width + index_from + first + u], lines) for u in range(BATCH)
            ]
            sums = [
                table_v[pl.ds(places[u], lines), :] + source_v[pl.ds(place + u * lines, lines), :]
                for u in range(BATCH)
            ]
            for u in range(BATCH):
                table_v[pl.ds(places[u], lines), :] = sums[u]
            return carry

        lax.fori_loop(start, stop, add, 0)

    copies = []
    for q in range(pieces):

        def block(b, carry):
            start = index_ref[b * width + facts_at + 1 + q] if q else 0
            add_rows(wide_v, b, keep, 0, start, index_ref[b * width + facts_at + 2 + q])
            if spilled:
                start = index_ref[b * width + facts_at + (1 + pieces + q if q else 1)]
                add_rows(
                    over_v, b, spilled, facts_at - LANES, start,
                    index_ref[b * width + facts_at + 2 + pieces + q],
                )
            return carry

        lax.fori_loop(0, blocks, block, 0)
        rows = pl.ds(q * span, span)
        copies.append(pltpu.make_async_copy(table_v.at[rows], out_ref.at[rows], sem.at[q]))
        copies[q].start()
    for copy in copies:
        copy.wait()


def table(index, rows, over, block_rows):
    n, stacks, keep, half = rows.shape
    lines = half // LANES
    blocks = n * stacks
    pieces = pieces_of(block_rows)
    spilled = 0 if over is None else over.shape[2]
    vmem = pl.BlockSpec(memory_space=pltpu.VMEM)
    operands = [index.reshape(-1), rows.reshape(blocks, keep, half)]
    any_space = pl.BlockSpec(memory_space=pl.ANY)
    in_specs = [pl.BlockSpec(memory_space=pltpu.SMEM), any_space]
    scratch = [pltpu.VMEM((blocks, keep, half), jnp.bfloat16)]
    scratch += [pltpu.VMEM((blocks * keep * lines, LANES), jnp.float32)]
    if spilled:
        operands.append(over.reshape(blocks, spilled, half))
        in_specs.append(vmem)
        scratch.append(pltpu.VMEM((blocks * spilled * lines, LANES), jnp.float32))
    scratch.append(pltpu.VMEM(((block_rows + 1) * lines, LANES), jnp.float32))
    scratch += [pltpu.SemaphoreType.DMA((pieces,)), pltpu.SemaphoreType.DMA]
    return pl.pallas_call(
        functools.partial(table_kernel, spilled, index.shape[-1], pieces),
        out_shape=jax.ShapeDtypeStruct((block_rows * lines, LANES), jnp.float32),
        in_specs=in_specs,
        out_specs=any_space,
        scratch_shapes=scratch,
        compiler_params=pltpu.CompilerParams(vmem_limit_bytes=VMEM_LIMIT),
    )(*operands)


def on_device(token_ids, embedded, norm_gain, proj_grad, proj_weight, stream_grad):
    n = lax.axis_size("dp")
    tokens = token_ids.shape[1]
    cap = max(2, 2 * tokens // n)
    block_rows = VOCAB // n
    tiers = cap == LANES
    keep = 3 * cap // 8 if tiers else cap
    spill = 9 * cap // 16 if tiers else 0
    rows, index, over, kept = exchange(
        token_ids, embedded[0], norm_gain, proj_grad[0], proj_weight[0], stream_grad[0],
        n, lax.axis_size("mp"), cap, keep, spill, block_rows,
    )
    half = rows.shape[-1]
    if tiers:

        def whole():
            full_rows, full_index = full_exchange(token_ids, kept, n, cap, block_rows)
            return table(full_index, full_rows, None, block_rows)

        def short():
            return table(index, rows, over, block_rows)

        out = lax.cond(jnp.max(index[:, :, 0, index.shape[-1] - LANES]) > 0, whole, short)
    else:
        out = table(index, rows, None, block_rows)
    return out.reshape(block_rows, 1, half)


def solution(mesh):
    return jax.shard_map(
        on_device,
        mesh=mesh,
        in_specs=(
            P("pipe", "dp"),
            P("pipe", "dp", "mp"),
            P("pipe", "mp"),
            P("pipe", "dp", None),
            P("pipe", "mp", None),
            P("pipe", "dp", "mp"),
        ),
        out_specs=P("dp", "mp", "pipe"),
        check_vma=False,
    )
```

```python
import functools

import jax
import jax.numpy as jnp
from jax import lax
from jax.experimental import pallas as pl
from jax.experimental.pallas import tpu as pltpu
from jax.sharding import PartitionSpec as P

VOCAB = 32128
LANES = 128
epsilon = 1e-06
BATCH = 8
VMEM_LIMIT = 60 * 1024 * 1024


def partner(me, k, n):
    out, bit = 0, 1
    while bit < n:
        mine = (me // bit) % 2
        flip = (k // bit) % 2
        out = out + bit * (mine + flip - 2 * mine * flip)
        bit *= 2
    return out


def contract_last(a, b):
    return lax.dot_general(a, b, (((1,), (1,)), ((), ())), preferred_element_type=jnp.float32)


def greet_all(n, pipe, other, me, mp):
    barrier = pltpu.get_barrier_semaphore()

    def greet(k, carry):
        d = partner(me, k, n)
        pl.semaphore_signal(
            barrier, inc=1, device_id={"dp": d, "pipe": other}, device_id_type=pl.DeviceIdType.MESH
        )

        @pl.when(k > 0)
        def _():
            pl.semaphore_signal(
                barrier, inc=1, device_id={"dp": d, "pipe": pipe}, device_id_type=pl.DeviceIdType.MESH
            )

        return carry

    lax.fori_loop(0, n, greet, 0)
    if mp is not None:
        pl.semaphore_signal(
            barrier, inc=1, device_id={"mp": 1 - mp}, device_id_type=pl.DeviceIdType.MESH
        )
    return barrier


def pieces_of(block_rows):
    pieces = 8
    while block_rows % pieces:
        pieces //= 2
    return pieces


def index_lanes(keep):
    return -(-keep // LANES) * LANES


def batches(count):
    return jnp.floor((count + (BATCH - 1)) * (1.0 / BATCH))


def find_places(n, keep, spill, block_rows, me, ids_ref, placer_v, local_v, facts_v):
    tokens = ids_ref.shape[1]
    ids = ids_ref[...].astype(jnp.float32)
    ids_down = jnp.broadcast_to(ids, (LANES, tokens)).T[:, 0:1]
    earlier = lax.broadcasted_iota(jnp.int32, (tokens, tokens), 0) < lax.broadcasted_iota(
        jnp.int32, (tokens, tokens), 1
    )
    same = jnp.where((ids_down == ids) & earlier, 1.0, 0.0)
    first = jnp.where(jnp.sum(same, axis=0, keepdims=True) > 0.0, 0.0, 1.0)
    first_down = jnp.broadcast_to(first, (LANES, tokens)).T[:, 0:1]
    rank = jnp.sum(jnp.where(ids_down < ids, first_down, 0.0), axis=0, keepdims=True)

    k = lax.broadcasted_iota(jnp.int32, (n, 1), 0)
    low = (partner(me, k, n) * block_rows).astype(jnp.float32)

    def below(edge):
        return jnp.sum(jnp.where(ids < edge, first, 0.0), axis=1, keepdims=True)

    pieces = pieces_of(block_rows)
    base = below(low)
    bounds = [below(low + float(q * (block_rows // pieces))) - base for q in range(1, pieces + 1)]
    match = jnp.where((ids >= low) & (ids < low + float(block_rows)), 1.0, 0.0)
    rank = rank - jnp.sum(match * base, axis=0, keepdims=True)
    slot = jnp.sum(match * (k * keep).astype(jnp.float32), axis=0, keepdims=True)
    local = ids - jnp.sum(match * low, axis=0, keepdims=True)
    position = jnp.where(rank < keep, slot + rank, -1.0)
    lane = lax.broadcasted_iota(jnp.int32, (n, LANES), 1)
    facts = jnp.zeros((n, LANES), jnp.float32)
    for q in range(pieces):
        facts = jnp.where(lane == 2 + q, batches(jnp.minimum(bounds[q], keep)), facts)
    if spill:
        over = jnp.maximum(bounds[-1] - keep, 0.0)
        start = jnp.zeros((n, 1), jnp.float32)
        for o in range(n):
            start = start + jnp.where(k > o, over[o:o + 1], 0.0)
        behind = jnp.sum(match * start, axis=0, keepdims=True) + (rank + (n * keep - keep))
        position = jnp.where(rank < keep, position, behind)
        full = jnp.where(jnp.sum(over, axis=0, keepdims=True) > spill, 1.0, 0.0)
        begin = jnp.floor(start * (1.0 / BATCH))
        facts = jnp.where(lane == 0, full, jnp.where(lane == 1, begin, facts))
        for q in range(pieces):
            passed = jnp.maximum(bounds[q] - keep, 0.0)
            passed = jnp.where(passed > 0.0, batches(start + passed), begin)
            facts = jnp.where(lane == 2 + pieces + q, jnp.minimum(passed, float(spill // BATCH)), facts)
    facts_v[...] = facts.astype(jnp.int32)
    high = jnp.floor(local * (1.0 / 64.0))
    row = lax.broadcasted_iota(jnp.int32, (8, tokens), 0)
    parts = jnp.where(row == 0, high, jnp.where(row == 1, local - high * 64.0, 0.0))
    owner = jnp.sum(match * (k + 1).astype(jnp.float32), axis=0, keepdims=True)
    parts = jnp.where(row == 2, owner, parts) * first
    local_v[...] = parts.astype(jnp.bfloat16)
    slots = lax.broadcasted_iota(jnp.int32, placer_v.shape, 0)
    placer_v[...] = jnp.where(position.astype(jnp.int32) == slots, 1.0, 0.0).astype(jnp.bfloat16)


def place_indices(n, keep, spill, block_rows, lines, placer_v, local_v, facts_v, sendi_v):
    parts = contract_last(local_v[...], placer_v[...])
    owner = parts[2:3]
    found = parts[0:1] * 64.0 + parts[1:2]
    found = jnp.where(owner > 0.0, found, float(block_rows))
    found = (found * float(lines)).astype(jnp.int32)
    facts_at = sendi_v.shape[2] - LANES
    sendi_v[...] = jnp.zeros(sendi_v.shape, jnp.int32)
    for k in range(n):
        sendi_v[k, :, 0:keep] = found[:, k * keep:(k + 1) * keep]
        if spill:
            sendi_v[k, :, facts_at - LANES:facts_at] = jnp.where(
                owner[:, n * keep:] == float(k + 1), found[:, n * keep:], block_rows * lines
            )
        sendi_v[k, :, facts_at:] = facts_v[k:k + 1, :]


def place_rows(p, first, chunk, keep, spill, placer_v, part, send_v, over_v):
    n = send_v.shape[0]
    cols = pl.ds(first, chunk)
    placed = jnp.dot(
        placer_v[0:n * keep + spill, :], part, preferred_element_type=jnp.float32
    ).astype(jnp.bfloat16)
    send_v[:, p, :, cols] = placed[:n * keep].reshape(n, keep, chunk)
    if spill:
        over_v[p, :, cols] = placed[n * keep:]


def remote(src, dst, send_sem, recv_sem, **where):
    return pltpu.make_async_remote_copy(
        src_ref=src, dst_ref=dst, send_sem=send_sem, recv_sem=recv_sem,
        device_id=where, device_id_type=pl.DeviceIdType.MESH,
    )


def make_sender(n, pipe, other, me, send_v, sendi_v, rows_out, index_out, sems):
    send_sem, recv_sem, isend_sem, irecv_sem = sems

    def copies(k, p, s):
        d = partner(me, k, n)
        return (
            remote(send_v.at[k, p], rows_out.at[k, s], send_sem.at[k, p], recv_sem.at[k, s], dp=d, pipe=p),
            remote(sendi_v.at[k], index_out.at[k, s], isend_sem.at[k, p], irecv_sem.at[k, s], dp=d, pipe=p),
        )

    def send(k, own_chip):
        copies(k, other, pipe)[0].start()
        if not own_chip:
            copies(k, pipe, pipe)[0].start()

    def send_indices():
        def send_index(k, carry):
            copies(k, other, pipe)[1].start()
            copies(k, pipe, pipe)[1].start()
            return carry

        lax.fori_loop(1, n, send_index, 0)
        copies(0, other, pipe)[1].start()

    def arrive(k, carry):
        for copy in copies(k, other, pipe):
            copy.wait_send()
        for copy in copies(k, other, other):
            copy.wait_recv()

        @pl.when(k > 0)
        def _():
            for copy in copies(k, pipe, pipe):
                copy.wait_send()
            for copy in copies(k, other, pipe):
                copy.wait_recv()

        return carry

    return send_indices, send, arrive


def exchange_kernel(
    n, cap, keep, spill, block_rows, full_width, chunk,
    ids_ref, gain_ref, embedded, proj_grad, weight, stream,
    rows_out, index_out, spill_out, kept_out,
    emb_v, grad_v, weight_v, stream_v, scaled_v, rows_v, send_v, sendi_v, over_v, sums_v, sums_got,
    placer_v, local_v, facts_v,
    in_sem, weight_sem, sum_send, sum_recv, send_sem, recv_sem, isend_sem, irecv_sem, own_sem,
    pair_send, pair_recv, line_send, line_recv, side_send, side_recv,
):
    pipe = lax.axis_index("pipe")
    me = lax.axis_index("dp")
    mp = lax.axis_index("mp")
    other = 1 - pipe
    tokens, width = emb_v.shape
    half = width // 2

    loads = [
        pltpu.make_async_copy(proj_grad, grad_v, in_sem.at[0]),
        pltpu.make_async_copy(embedded, emb_v, in_sem.at[1]),
        pltpu.make_async_copy(stream, stream_v, in_sem.at[2]),
    ]
    chunks = [
        pltpu.make_async_copy(
            weight.at[pl.ds(j * chunk, chunk)], weight_v.at[pl.ds(j * chunk, chunk)], weight_sem.at[j]
        )
        for j in range(width // chunk)
    ]
    loads[0].start()
    chunks[0].start()
    barrier = greet_all(n, pipe, other, me, mp)
    find_places(n, keep, spill, block_rows, me, ids_ref, placer_v, local_v, facts_v)
    chunks[1].start()
    loads[1].start()

    loads[0].wait()
    mixed = jnp.zeros((tokens, 1), jnp.float32)
    square = jnp.zeros((tokens, 1), jnp.float32)
    for j in range(width // chunk):
        cols = pl.ds(j * chunk, chunk)
        if j + 2 < width // chunk:
            chunks[j + 2].start()
        else:
            loads[2].start() if j + 2 == width // chunk else None
        chunks[j].wait()
        scaled = contract_last(grad_v[...], weight_v[cols, :]) * gain_ref[:, cols]
        scaled_v[:, cols] = scaled
        if j == 0:
            loads[1].wait()
        inputs = emb_v[:, cols].astype(jnp.float32)
        square = square + jnp.sum(inputs * inputs, axis=1, keepdims=True)
        mixed = mixed + jnp.sum(inputs * scaled, axis=1, keepdims=True)
    lane = lax.broadcasted_iota(jnp.int32, (tokens, LANES), 1)
    packed = jnp.where(lane == 0, square, jnp.where(lane == 1, mixed, 0.0))
    sums_v[...] = packed.T[:8]

    pl.semaphore_wait(barrier, 2 * n)
    swap = remote(sums_v, sums_got, sum_send, sum_recv, mp=1 - mp)
    swap.start()
    place_indices(n, keep, spill, block_rows, half // LANES, placer_v, local_v, facts_v, sendi_v)
    send_indices, send, arrive = make_sender(
        n, pipe, other, me, send_v, sendi_v, rows_out, index_out,
        (send_sem, recv_sem, isend_sem, irecv_sem),
    )
    send_indices()
    loads[2].wait()
    swap.wait()

    total = sums_v[...] + sums_got[...]
    inverse = lax.rsqrt(total[0:1] / full_width + epsilon)
    coef = inverse * inverse * inverse * total[1:2] / full_width
    line = lax.broadcasted_iota(jnp.int32, (LANES, tokens), 0)
    back = jnp.where(line == 0, inverse, jnp.where(line == 1, coef, 0.0)).T
    if spill:
        pair = remote(over_v.at[other], spill_out.at[0, pipe], pair_send, pair_recv, pipe=other)
    for h in range(2):
        p = pipe if h else other
        for first in range(0, half, chunk):
            cols = pl.ds(pl.multiple_of(p * half + first, chunk), chunk)
            norm_back = back[:, 0:1] * scaled_v[:, cols] - emb_v[:, cols].astype(jnp.float32) * back[:, 1:2]
            part = (stream_v[:, cols].astype(jnp.float32) + norm_back).astype(jnp.bfloat16)
            if spill:
                rows_v[:, cols] = part
            place_rows(p, first, chunk, keep, spill, placer_v, part, send_v, over_v)
        if spill and h == 0:
            pair.start()

    if spill:
        lines = n // 2
        at, beside = me // 2, partner(me, 1, n)
        own_over = pltpu.make_async_copy(over_v.at[pipe], spill_out.at[0, pipe], own_sem.at[2])
        own_over.start()
        kept = pltpu.make_async_copy(rows_v, kept_out, own_sem.at[3])
        kept.start()

        def along(up, r, source, to):
            return remote(
                spill_out.at[partner(me, source, n)], spill_out.at[partner(to, source, n)],
                line_send.at[up, r], line_recv.at[up, r], dp=to,
            )

        def across(source):
            return remote(
                spill_out.at[partner(me, source, n)], spill_out.at[partner(beside, source, n)],
                side_send.at[source // 2], side_recv.at[source // 2], dp=beside,
            )

        def pass_on(r):
            for up in (1, 0):
                step = 2 if up else -2
                source = me - step * r
                here = (at >= r) if up else (at + r < lines)
                more = (at + 1 < lines) if up else (at >= 1)
                if r > 0:

                    @pl.when(here)
                    def _():
                        remote(
                            spill_out.at[0], spill_out.at[partner(me, source, n)],
                            line_send.at[up, r], line_recv.at[up, r], dp=beside,
                        ).wait_recv()
                        across(source).start()

                @pl.when(here & more)
                def _():
                    along(up, r + 1, source, me + step).start()

            if r == 0:
                across(me).start()

        def finish(r):
            for up in (1, 0):
                step = 2 if up else -2
                source = me - step * r
                here = (at >= r) if up else (at + r < lines)
                more = (at + 1 < lines) if up else (at >= 1)

                @pl.when(here & more)
                def _():
                    along(up, r + 1, source, me + step).wait_send()

        send(1, False)
        own_over.wait()
        pair.wait()
        pass_on(0)
        send(2, False)
        send(3, False)
        pass_on(1)
        send(6, False)
        send(7, False)
        pass_on(2)
        send(4, False)
        send(5, False)
        pass_on(3)
        send(0, True)
    else:

        def send_on(k, carry):
            send(k, False)
            return carry

        lax.fori_loop(1, n, send_on, 0)
        send(0, True)
    own_rows = pltpu.make_async_copy(send_v.at[0, pipe], rows_out.at[0, pipe], own_sem.at[0])
    own_index = pltpu.make_async_copy(sendi_v.at[0], index_out.at[0, pipe], own_sem.at[1])
    own_rows.start()
    own_index.start()
    lax.fori_loop(0, n, arrive, 0)
    own_rows.wait()
    own_index.wait()
    if spill:
        for r in range(lines):
            finish(r)

        def side(z, carry):
            remote(
                spill_out.at[partner(me, 2 * z, n)], spill_out.at[partner(me, 2 * z + beside % 2, n)],
                side_send.at[z], side_recv.at[z], dp=beside,
            ).wait()
            return carry

        lax.fori_loop(0, lines, side, 0)
        kept.wait()


def exchange(ids, embedded, gain, proj_grad, weight, stream, n, n_mp, cap, keep, spill, block_rows):
    tokens, width = embedded.shape
    inner = proj_grad.shape[1]
    half = width // 2
    chunk = min(512, half)
    index_width = index_lanes(keep) + (2 * LANES if spill else LANES)
    over = (spill or 16, half)
    kept = (tokens, width) if spill else (8, LANES)
    any_space = pl.BlockSpec(memory_space=pl.ANY)
    vmem = pl.BlockSpec(memory_space=pltpu.VMEM)
    dma = pltpu.SemaphoreType.DMA
    return pl.pallas_call(
        functools.partial(exchange_kernel, n, cap, keep, spill, block_rows, width * n_mp, chunk),
        out_shape=(
            jax.ShapeDtypeStruct((n, 2, keep, half), jnp.bfloat16),
            jax.ShapeDtypeStruct((n, 2, 1, index_width), jnp.int32),
            jax.ShapeDtypeStruct((n if spill else 1, 2) + over, jnp.bfloat16),
            jax.ShapeDtypeStruct(kept, jnp.bfloat16),
        ),
        in_specs=[vmem, vmem] + [any_space] * 4,
        out_specs=(any_space,) * 4,
        scratch_shapes=[
            pltpu.VMEM((tokens, width), jnp.bfloat16),
            pltpu.VMEM((tokens, inner), jnp.bfloat16),
            pltpu.VMEM((width, inner), jnp.bfloat16),
            pltpu.VMEM((tokens, width), jnp.bfloat16),
            pltpu.VMEM((tokens, width), jnp.float32),
            pltpu.VMEM((tokens, width), jnp.bfloat16),
            pltpu.VMEM((n, 2, keep, half), jnp.bfloat16),
            pltpu.VMEM((n, 1, index_width), jnp.int32),
            pltpu.VMEM((2,) + over, jnp.bfloat16),
            pltpu.VMEM((8, tokens), jnp.float32),
            pltpu.VMEM((8, tokens), jnp.float32),
            pltpu.VMEM((n * keep + (LANES if spill else 0), tokens), jnp.bfloat16),
            pltpu.VMEM((8, tokens), jnp.bfloat16),
            pltpu.VMEM((n, LANES), jnp.int32),
            dma((3,)),
            dma((width // chunk,)),
            dma,
            dma,
            dma((n, 2)),
            dma((n, 2)),
            dma((n, 2)),
            dma((n, 2)),
            dma((4,)),
            dma,
            dma,
            dma((2, n)),
            dma((2, n)),
            dma((n,)),
            dma((n,)),
        ],
        compiler_params=pltpu.CompilerParams(
            collective_id=0, has_side_effects=True, vmem_limit_bytes=VMEM_LIMIT
        ),
    )(ids, gain, embedded, proj_grad, weight, stream)


def full_kernel(
    n, cap, block_rows, ids_ref, rows_v, rows_out, index_out, send_v, sendi_v, placer_v, local_v, facts_v,
    send_sem, recv_sem, isend_sem, irecv_sem, own_sem,
):
    pipe = lax.axis_index("pipe")
    me = lax.axis_index("dp")
    other = 1 - pipe
    barrier = greet_all(n, pipe, other, me, None)
    pl.semaphore_wait(barrier, 2 * n - 1)
    find_places(n, cap, 0, block_rows, me, ids_ref, placer_v, local_v, facts_v)
    width = rows_v.shape[1]
    place_indices(n, cap, 0, block_rows, width // 2 // LANES, placer_v, local_v, facts_v, sendi_v)
    chunk = min(256, width // 2)
    for c in range(width // chunk):
        place_rows(
            c * chunk // (width // 2), c * chunk % (width // 2), chunk, cap, 0, placer_v,
            rows_v[:, c * chunk:(c + 1) * chunk], send_v, None,
        )
    send_indices, send, arrive = make_sender(
        n, pipe, other, me, send_v, sendi_v, rows_out, index_out,
        (send_sem, recv_sem, isend_sem, irecv_sem),
    )
    send_indices()

    def send_on(k, carry):
        send(k, False)
        return carry

    lax.fori_loop(1, n, send_on, 0)
    send(0, True)
    own_rows = pltpu.make_async_copy(send_v.at[0, pipe], rows_out.at[0, pipe], own_sem.at[0])
    own_index = pltpu.make_async_copy(sendi_v.at[0], index_out.at[0, pipe], own_sem.at[1])
    own_rows.start()
    own_index.start()
    lax.fori_loop(0, n, arrive, 0)
    own_rows.wait()
    own_index.wait()


def full_exchange(ids, rows, n, cap, block_rows):
    tokens, width = rows.shape
    half = width // 2
    any_space = pl.BlockSpec(memory_space=pl.ANY)
    vmem = pl.BlockSpec(memory_space=pltpu.VMEM)
    dma = pltpu.SemaphoreType.DMA
    return pl.pallas_call(
        functools.partial(full_kernel, n, cap, block_rows),
        out_shape=(
            jax.ShapeDtypeStruct((n, 2, cap, half), jnp.bfloat16),
            jax.ShapeDtypeStruct((n, 2, 1, index_lanes(cap) + LANES), jnp.int32),
        ),
        in_specs=[vmem, vmem],
        out_specs=(any_space, any_space),
        scratch_shapes=[
            pltpu.VMEM((n, 2, cap, half), jnp.bfloat16),
            pltpu.VMEM((n, 1, index_lanes(cap) + LANES), jnp.int32),
            pltpu.VMEM((n * cap, tokens), jnp.bfloat16),
            pltpu.VMEM((8, tokens), jnp.bfloat16),
            pltpu.VMEM((n, LANES), jnp.int32),
            dma((n, 2)),
            dma((n, 2)),
            dma((n, 2)),
            dma((n, 2)),
            dma((2,)),
        ],
        compiler_params=pltpu.CompilerParams(
            collective_id=1, has_side_effects=True, vmem_limit_bytes=VMEM_LIMIT
        ),
    )(ids, rows)


def table_kernel(spilled, width, pieces, index_ref, rows_ref, *rest):
    if spilled:
        over_ref, out_ref, rows_v, wide_v, over_v, table_v, sem, in_sem = rest
    else:
        out_ref, rows_v, wide_v, table_v, sem, in_sem = rest
    blocks, keep, half = rows_ref.shape
    load = pltpu.make_async_copy(rows_ref, rows_v, in_sem)
    load.start()
    lines = half // LANES
    span = out_ref.shape[0] // pieces
    facts_at = width - LANES
    parts = 16
    while out_ref.shape[0] % (8 * parts):
        parts //= 2
    clear_rows = out_ref.shape[0] // parts

    def clear(i, carry):
        table_v[pl.ds(pl.multiple_of(i * clear_rows, 8), clear_rows), :] = jnp.zeros(
            (clear_rows, LANES), jnp.float32
        )
        return carry

    lax.fori_loop(0, parts, clear, 0)
    load.wait()

    def widen(b, carry):
        for j in range(lines):
            wide_v[pl.ds(b * keep * lines + j, keep, stride=lines), :] = rows_v[
                b, :, j * LANES:(j + 1) * LANES
            ].astype(jnp.float32)
        if spilled:

            @pl.when(index_ref[b * width + facts_at + 1 + 2 * pieces] > index_ref[b * width + facts_at + 1])
            def _():
                for j in range(lines):
                    over_v[pl.ds(b * spilled * lines + j, spilled, stride=lines), :] = over_ref[
                        b, :, j * LANES:(j + 1) * LANES
                    ].astype(jnp.float32)

        return carry

    lax.fori_loop(0, blocks, widen, 0)

    def add_rows(source_v, b, size, index_from, start, stop):
        def add(g, carry):
            first = g * BATCH
            place = pl.multiple_of((b * size + first) * lines, BATCH * lines)
            places = [
                pl.multiple_of(index_ref[b * width + index_from + first + u], lines) for u in range(BATCH)
            ]
            sums = [
                table_v[pl.ds(places[u], lines), :] + source_v[pl.ds(place + u * lines, lines), :]
                for u in range(BATCH)
            ]
            for u in range(BATCH):
                table_v[pl.ds(places[u], lines), :] = sums[u]
            return carry

        lax.fori_loop(start, stop, add, 0)

    copies = []
    for q in range(pieces):

        def block(b, carry):
            start = index_ref[b * width + facts_at + 1 + q] if q else 0
            add_rows(wide_v, b, keep, 0, start, index_ref[b * width + facts_at + 2 + q])
            if spilled:
                start = index_ref[b * width + facts_at + (1 + pieces + q if q else 1)]
                add_rows(
                    over_v, b, spilled, facts_at - LANES, start,
                    index_ref[b * width + facts_at + 2 + pieces + q],
                )
            return carry

        lax.fori_loop(0, blocks, block, 0)
        rows = pl.ds(q * span, span)
        copies.append(pltpu.make_async_copy(table_v.at[rows], out_ref.at[rows], sem.at[q]))
        copies[q].start()
    for copy in copies:
        copy.wait()


def table(index, rows, over, block_rows):
    n, stacks, keep, half = rows.shape
    lines = half // LANES
    blocks = n * stacks
    pieces = pieces_of(block_rows)
    spilled = 0 if over is None else over.shape[2]
    vmem = pl.BlockSpec(memory_space=pltpu.VMEM)
    operands = [index.reshape(-1), rows.reshape(blocks, keep, half)]
    any_space = pl.BlockSpec(memory_space=pl.ANY)
    in_specs = [pl.BlockSpec(memory_space=pltpu.SMEM), any_space]
    scratch = [pltpu.VMEM((blocks, keep, half), jnp.bfloat16)]
    scratch += [pltpu.VMEM((blocks * keep * lines, LANES), jnp.float32)]
    if spilled:
        operands.append(over.reshape(blocks, spilled, half))
        in_specs.append(vmem)
        scratch.append(pltpu.VMEM((blocks * spilled * lines, LANES), jnp.float32))
    scratch.append(pltpu.VMEM(((block_rows + 1) * lines, LANES), jnp.float32))
    scratch += [pltpu.SemaphoreType.DMA((pieces,)), pltpu.SemaphoreType.DMA]
    return pl.pallas_call(
        functools.partial(table_kernel, spilled, index.shape[-1], pieces),
        out_shape=jax.ShapeDtypeStruct((block_rows * lines, LANES), jnp.float32),
        in_specs=in_specs,
        out_specs=any_space,
        scratch_shapes=scratch,
        compiler_params=pltpu.CompilerParams(vmem_limit_bytes=VMEM_LIMIT),
    )(*operands)


def on_device(token_ids, embedded, norm_gain, proj_grad, proj_weight, stream_grad):
    n = lax.axis_size("dp")
    tokens = token_ids.shape[1]
    cap = max(2, 2 * tokens // n)
    block_rows = VOCAB // n
    tiers = cap == LANES
    keep = 3 * cap // 8 if tiers else cap
    spill = 9 * cap // 16 if tiers else 0
    rows, index, over, kept = exchange(
        token_ids, embedded[0], norm_gain, proj_grad[0], proj_weight[0], stream_grad[0],
        n, lax.axis_size("mp"), cap, keep, spill, block_rows,
    )
    half = rows.shape[-1]
    if tiers:

        def whole():
            full_rows, full_index = full_exchange(token_ids, kept, n, cap, block_rows)
            return table(full_index, full_rows, None, block_rows)

        def short():
            return table(index, rows, over, block_rows)

        out = lax.cond(jnp.max(index[:, :, 0, index.shape[-1] - LANES]) > 0, whole, short)
    else:
        out = table(index, rows, None, block_rows)
    return out.reshape(block_rows, 1, half)


def solution(mesh):
    return jax.shard_map(
        on_device,
        mesh=mesh,
        in_specs=(
            P("pipe", "dp"),
            P("pipe", "dp", "mp"),
            P("pipe", "mp"),
            P("pipe", "dp", None),
            P("pipe", "mp", None),
            P("pipe", "dp", "mp"),
        ),
        out_specs=P("dp", "mp", "pipe"),
        check_vma=False,
    )
```
